256 devices in a mesh: store: 16 (over x, y_hi, core), tp: 16 (over y_lo, z).
Axes of the slice: x: 4, y: 4 (y_hi: 2, y_lo: 2; y = y_hi * 2 + y_lo), z: 8, core: 2. Of those that a mesh axis runs over, the one named last changes fastest.
Arguments:
- hidden: bfloat16 [16, 576, 8192], P('store', None, 'tp'), may hold values from -300 to 300
- w_query: bfloat16 [8192, 4096], P(None, 'tp'), may hold values from -0.0625 to 0.0625
- w_keyvalue: bfloat16 [8192, 1024], P('tp'), may hold values from -0.1875 to 0.1875
- passage_cache: bfloat16 [64, 4, 384, 256], P('store'), may hold values from -400 to 400
- passage_ids: int32 [16, 8], replicated, may hold values from 0 to 63, as said below
- select_index: int32 [16, 576], P('store'), may hold values from 0 to 3071, as said below
- select_count: int32 [16], P('store'), may hold values from 288 to 576, as said below
Outputs:
- context: bfloat16 [16, 576, 4096], P('store', None, 'tp')
The draws below stay inside these ranges and needn't reach their ends.
Inputs may be any that keep to these rules, and one draw needn't show every extreme that they name: `passage_ids`: the passages of one prompt lie in distinct shards of the pool, shard = id // 4. `select_index`: all entries of a row are distinct positions of the prompt; the first select_count[p] of row p are in increasing order, the others are ignored. `select_count`: some prompt of every draw has 576 selected tokens.
All inputs are finite; a program needn't handle non-finite values.
Results may differ from the reference program's by a relative error of at most 0.04.
Values may be sent and summed in bfloat16 or wider, within the bound.
A program may use at most 128 MiB of HBM per device.

```python
import math
import jax
import jax.numpy as jnp
from jax import lax

D = 8192
HEADS = 32
KV_HEADS = 4
HEAD_DIM = 128
PASSAGE = 384
PASSAGES = 8
ROWS = 576
POOL_DEV = 4
SEQ = 3072
PROMPTS = 16
POOL = 64


def draw_hidden(key, part):
    split = jax.random.split(jax.random.fold_in(key, 11), 3)
    noise = jnp.clip(jax.random.normal(split[0], (PROMPTS, ROWS, D), jnp.float32), -4.0, 4.0)
    row_scale = jnp.exp(jax.random.uniform(split[1], (PROMPTS, ROWS, 1), jnp.float32, 0.0, math.log(10.0)))
    column_scale = jnp.exp(jax.random.uniform(split[2], (D,), jnp.float32, math.log(0.5), math.log(5.0)))
    return (noise * row_scale * column_scale).astype(jnp.bfloat16)


def draw_passage_cache(key, part):
    split = jax.random.split(jax.random.fold_in(key, 13), 1)
    shape = (POOL, KV_HEADS, PASSAGE, 2 * HEAD_DIM)
    result = 2.0 * jnp.clip(jax.random.normal(split[0], shape, jnp.float32), -4.0, 4.0)
    return result.astype(jnp.bfloat16)


def owner_draw(subkey):
    return jax.random.permutation(subkey, PROMPTS)[:PASSAGES]


def draw_passage_ids(key, part):
    split = jax.random.split(jax.random.fold_in(key, 17), 3)
    owners = jax.vmap(owner_draw)(jax.random.split(split[0], PROMPTS)).astype(jnp.int32)
    first_pick = jax.random.randint(split[1], (PROMPTS, PASSAGES), 0, POOL_DEV)
    second_pick = jax.random.randint(split[2], (PROMPTS, PASSAGES), 0, POOL_DEV)
    local_index = jnp.minimum(first_pick, second_pick)
    return (owners * POOL_DEV + local_index).astype(jnp.int32)


def selection(key):
    split = jax.random.split(jax.random.fold_in(key, 19), 3)
    counts = jax.random.randint(split[0], (PROMPTS,), ROWS // 2, ROWS + 1)
    fullest = jax.random.randint(split[1], (), 0, PROMPTS)
    counts = jnp.where(jnp.arange(PROMPTS) == fullest, ROWS, counts).astype(jnp.int32)
    ranking = jax.random.randint(split[2], (PROMPTS, SEQ), 0, 2 ** 30 // SEQ) * SEQ + jnp.arange(SEQ)
    picked = lax.top_k(ranking, ROWS)[1].astype(jnp.int32)
    order_key = jnp.where(jnp.arange(ROWS)[None, :] < counts[:, None], picked, picked + SEQ)
    ordered = jnp.sort(order_key, axis=1)
    positions = jnp.where(ordered >= SEQ, ordered - SEQ, ordered)
    return (counts, positions.astype(jnp.int32))


def draw_select_index(key, part):
    return selection(key)[1]


def draw_select_count(key, part):
    return selection(key)[0]


def raised(drawn, rng, source, target, blocks, factor):
    owner, partner = [(jnp.arange(drawn.shape[position]) // (drawn.shape[position] // blocks)).reshape([-1 if axis == position else 1 for axis in range(drawn.ndim)]) for position in (source, target)]
    chosen = jax.random.permutation(rng, blocks)[partner]
    strong = (owner == chosen) | (owner == (partner + blocks // 2) % blocks)
    return jnp.where(strong, factor * drawn, drawn)


def block_levels(rng, shape, cuts, low, largest):
    loudness = 1.0
    for position, parts in cuts:
        draws = jax.random.uniform(jax.random.fold_in(jax.random.fold_in(rng, 6), position), (parts,), jnp.float32, low / len(cuts), largest / len(cuts))
        loudness = loudness * jnp.repeat(jnp.exp(draws), shape[position] // parts).reshape((-1,) + (1,) * (len(shape) - 1 - position))
    return loudness


def gaussian(stream_key, extent, scale, most, cuts=(), kind=jnp.bfloat16):
    values = scale * jax.random.normal(stream_key, extent, jnp.float32)
    if cuts:
        values = values * block_levels(stream_key, extent, cuts, -0.22, 0.18)
    return jnp.clip(values, -most, most).astype(kind)


def gaussian_with(own_key, dims, width, limit, cuts, heavy, held_as=jnp.bfloat16):
    entries = width * jax.random.normal(own_key, dims, jnp.float32)
    if cuts:
        entries = entries * block_levels(own_key, dims, cuts, -0.22, 0.18)
    return jnp.clip(raised(entries, jax.random.fold_in(own_key, 3), *heavy), -limit, limit).astype(held_as)


def setup_inputs(seed: int = 0) -> dict:
    seeds = jax.random.split(jax.random.key(seed), 8)
    hidden = draw_hidden(jax.random.fold_in(seeds[7], 71), 0)
    w_query = gaussian(seeds[1], (D, HEADS * HEAD_DIM), D ** -0.5, 0.0625, ((1, 16),))
    w_keyvalue = gaussian_with(seeds[2], (D, KV_HEADS * 2 * HEAD_DIM), (D // 4) ** -0.5, 0.1875, ((0, 16),), (0, 1, 16, 2.0))
    passage_cache = draw_passage_cache(jax.random.fold_in(seeds[7], 71), 0)
    passage_ids = draw_passage_ids(jax.random.fold_in(seeds[7], 71), 0)
    select_index = draw_select_index(jax.random.fold_in(seeds[7], 71), 0)
    select_count = draw_select_count(jax.random.fold_in(seeds[7], 71), 0)
    return dict(hidden=hidden, w_query=w_query, w_keyvalue=w_keyvalue, passage_cache=passage_cache, passage_ids=passage_ids, select_index=select_index, select_count=select_count)


ROPE_BASE = 1000000.0
EPSILON = 1e-06

def rotate(vectors, positions):
    half_dim = vectors.shape[-1] // 2
    frequency = ROPE_BASE ** (-(jnp.arange(half_dim, dtype=jnp.float32) * 2.0) / vectors.shape[-1])
    angles = positions.astype(jnp.float32)[..., None] * frequency
    cosine = jnp.cos(angles)
    sine_part = jnp.sin(angles)
    front_half = vectors[..., :half_dim]
    back_half = vectors[..., half_dim:]
    return jnp.concatenate([front_half * cosine - back_half * sine_part, back_half * cosine + front_half * sine_part], axis=-1)

def reference(hidden, w_query, w_keyvalue, passage_cache, passage_ids, select_index, select_count):
    group_size = HEADS // KV_HEADS

    def one_prompt(inputs):
        token_rows, block_list, positions, live_count = inputs
        proj_q = jnp.dot(token_rows, w_query, preferred_element_type=jnp.float32)
        proj_kv = jnp.dot(token_rows, w_keyvalue, preferred_element_type=jnp.float32)
        widened = token_rows.astype(jnp.float32)
        inverse_rms = lax.rsqrt(lax.optimization_barrier(jnp.mean(widened * widened, axis=-1)) + EPSILON)
        queries = rotate((proj_q * inverse_rms[:, None]).reshape(ROWS, HEADS, HEAD_DIM), positions[:, None])
        queries = (queries * HEAD_DIM ** (-0.5)).astype(jnp.bfloat16)
        key_value = (proj_kv * inverse_rms[:, None]).reshape(ROWS, KV_HEADS, 2 * HEAD_DIM)
        new_keys = rotate(key_value[..., :HEAD_DIM], positions[:, None]).astype(jnp.bfloat16)
        new_values = key_value[..., HEAD_DIM:].astype(jnp.bfloat16)
        stored = jnp.take(passage_cache, block_list, axis=0)
        offsets = (jnp.arange(PASSAGES) * PASSAGE).astype(jnp.int32)
        old_keys = rotate(stored[..., :HEAD_DIM].astype(jnp.float32), offsets[:, None, None]).astype(jnp.bfloat16)
        old_keys = jnp.transpose(old_keys, (0, 2, 1, 3)).reshape(SEQ, KV_HEADS, HEAD_DIM)
        old_values = jnp.transpose(stored[..., HEAD_DIM:], (0, 2, 1, 3)).reshape(SEQ, KV_HEADS, HEAD_DIM)
        row_ids = jnp.arange(ROWS, dtype=jnp.int32)
        target = jnp.where(row_ids < live_count, positions, SEQ).astype(jnp.int32)
        all_keys = old_keys.at[target].set(new_keys, mode='drop')
        all_values = old_values.at[target].set(new_values, mode='drop')
        allowed = jnp.arange(SEQ, dtype=jnp.int32)[None, :] <= positions[:, None]
        outputs = []
        for kv_head in range(KV_HEADS):
            head_queries = queries[:, kv_head * group_size:(kv_head + 1) * group_size].astype(jnp.float32)
            head_keys = all_keys[:, kv_head].astype(jnp.float32)
            head_values = all_values[:, kv_head].astype(jnp.float32)
            scores = jnp.einsum('rgd,sd->grs', head_queries, head_keys)
            scores = jnp.where(allowed[None], scores, -jnp.inf)
            row_max = lax.optimization_barrier(jnp.max(scores, axis=-1, keepdims=True))
            shifted = jnp.exp(scores - row_max)
            weight = (shifted / lax.optimization_barrier(jnp.sum(shifted, axis=-1, keepdims=True))).astype(jnp.bfloat16)
            outputs.append(jnp.einsum('grs,sd->rgd', weight.astype(jnp.float32), head_values))
        context = jnp.concatenate(outputs, axis=1)
        row_live = (row_ids < live_count)[:, None, None]
        context = jnp.where(row_live, context, 0.0)
        return context.reshape(ROWS, HEADS * HEAD_DIM).astype(jnp.bfloat16)
    return lax.map(one_prompt, (hidden, passage_ids, select_index, select_count))
```

```python
import functools
import math

import jax
import jax.numpy as jnp
from jax import lax
from jax.experimental import pallas as pl
from jax.experimental.pallas import tpu as pltpu
from jax.sharding import PartitionSpec as P

D = 8192
KV_HEADS = 4
HEAD_DIM = 128
PASSAGE = 384
PASSAGES = 8
SEQ = 3072
ROWS = 576
ROPE_BASE = 1000000.0
EPSILON = 1e-06
BLOCK = 144
NEG = -1e30
FAR = 1 << 20


def turned(vectors, cosine, sine):
    return vectors * cosine + pltpu.roll(vectors, HEAD_DIM // 2, 1) * sine


def turn_tables(positions):
    half = HEAD_DIM // 2
    frequency = ROPE_BASE ** (-(jnp.arange(half, dtype=jnp.float32) * 2.0) / HEAD_DIM)
    angles = positions.astype(jnp.float32)[..., None] * frequency
    cosine, sine = jnp.cos(angles), jnp.sin(angles)
    return jnp.concatenate([cosine, cosine, -sine, sine], axis=-1)


def attend_kernel(
    ids_sm, pos_sm, count_sm, q_ref, kv_ref, inv_ref, pos_ref, table_ref, old_table_ref,
    incoming_ref, out_ref, q_s, nk_s, nv_s, kk_s, vv_s, kp_s, acc_s,
):
    heads = q_ref.shape[1] // HEAD_DIM
    count = count_sm[0]
    inverse = inv_ref[:ROWS, :1]
    store = lax.axis_index("store")
    cosine, sine = table_ref[:, :HEAD_DIM], table_ref[:, HEAD_DIM:]
    scale = HEAD_DIM**-0.5 * math.log2(math.e)
    for h in range(heads):
        part = q_ref[:, h * HEAD_DIM : (h + 1) * HEAD_DIM].astype(jnp.float32) * inverse
        q_s[h] = (turned(part, cosine, sine) * scale).astype(jnp.bfloat16)
    fresh = kv_ref[:, :HEAD_DIM].astype(jnp.float32) * inverse
    nk_s[:ROWS] = turned(fresh, cosine, sine).astype(jnp.bfloat16)
    nk_s[ROWS:] = jnp.zeros_like(nk_s[ROWS:])
    nv_s[:ROWS, :HEAD_DIM] = (kv_ref[:, HEAD_DIM:].astype(jnp.float32) * inverse).astype(jnp.bfloat16)
    nv_s[ROWS:, :HEAD_DIM] = jnp.zeros_like(nv_s[ROWS:, :HEAD_DIM])
    nv_s[:, HEAD_DIM:] = jnp.ones_like(nv_s[:, HEAD_DIM:])
    row_ids = lax.broadcasted_iota(jnp.int32, (ROWS, 1), 0)
    marked = jnp.where(row_ids < count, pos_ref[...], -1)

    def prepare(k, carry):
        block = incoming_ref[ids_sm[store, k] // 4]
        table = old_table_ref[k]
        keys = block[:, :HEAD_DIM].astype(jnp.float32)
        kk_s[k] = turned(keys, table[:, :HEAD_DIM], table[:, HEAD_DIM:]).astype(jnp.bfloat16)
        vv_s[k, :, :HEAD_DIM] = block[:, HEAD_DIM:]
        vv_s[k, :, HEAD_DIM:] = jnp.ones_like(block[:, HEAD_DIM:])
        here = k * PASSAGE + lax.broadcasted_iota(jnp.int32, (1, PASSAGE), 1)
        hit = jnp.max(jnp.where(marked == here, FAR, 0), axis=0, keepdims=True)
        kp_s[k] = jnp.broadcast_to(jnp.maximum(here, hit), (8, PASSAGE))
        return carry

    lax.fori_loop(0, PASSAGES, prepare, 0)
    contract = (((1,), (1,)), ((), ()))
    for b in range(ROWS // BLOCK):
        low, high = b * BLOCK, (b + 1) * BLOCK
        rows = heads * BLOCK

        @pl.when(low >= count)
        def _():
            out_ref[low:high] = jnp.zeros_like(out_ref[low:high])

        @pl.when(low < count)
        def _():
            queries = q_s[:, low:high].reshape(rows, HEAD_DIM)
            width = -(-high // 128) * 128
            scores = lax.dot_general(
                queries, nk_s[:width], contract, preferred_element_type=jnp.float32
            )
            row_of = low + lax.broadcasted_iota(jnp.int32, (BLOCK, width), 0)
            key_of = lax.broadcasted_iota(jnp.int32, (BLOCK, width), 1)
            seen = jnp.concatenate([key_of <= row_of] * heads, axis=0)
            scores = jnp.where(seen, scores, NEG)
            top = jnp.max(scores, axis=1, keepdims=True)
            weight = jnp.exp2(scores - top).astype(jnp.bfloat16)
            acc_s[...] = jnp.dot(weight, nv_s[:width], preferred_element_type=jnp.float32)
            place = pos_ref[low:high]
            place = jnp.concatenate([place] * heads, axis=0)
            last = jnp.minimum(count, high) - 1

            def old(k, top):
                scores = lax.dot_general(
                    queries, kk_s[k], contract, preferred_element_type=jnp.float32
                )
                scores = jnp.where(kp_s[k, 0:1] <= place, scores, NEG)
                risen = jnp.maximum(top, jnp.max(scores, axis=1, keepdims=True))
                weight = jnp.exp2(scores - risen).astype(jnp.bfloat16)
                part = jnp.dot(weight, vv_s[k], preferred_element_type=jnp.float32)
                acc_s[...] = acc_s[...] * jnp.exp2(top - risen) + part
                return risen

            lax.fori_loop(0, pos_sm[0, last] // PASSAGE + 1, old, top)
            result = acc_s[:, :HEAD_DIM] / acc_s[:, HEAD_DIM:]
            live = low + lax.broadcasted_iota(jnp.int32, (BLOCK, HEAD_DIM), 0) < count
            for h in range(heads):
                piece = jnp.where(live, result[h * BLOCK : (h + 1) * BLOCK], 0.0)
                out_ref[low:high, h * HEAD_DIM : (h + 1) * HEAD_DIM] = piece.astype(jnp.bfloat16)


def attend(passage_ids, select_index, select_count, q_raw, kv_raw, inverse, table, incoming):
    heads = q_raw.shape[1] // HEAD_DIM
    old_table = turn_tables(jnp.arange(PASSAGES) * PASSAGE)[:, None]
    smem = pl.BlockSpec(memory_space=pltpu.SMEM)
    vmem = pl.BlockSpec(memory_space=pltpu.VMEM)
    return pl.pallas_call(
        attend_kernel,
        out_shape=jax.ShapeDtypeStruct((ROWS, q_raw.shape[1]), jnp.bfloat16),
        in_specs=[smem] * 3 + [vmem] * 7,
        out_specs=vmem,
        scratch_shapes=[
            pltpu.VMEM((heads, ROWS, HEAD_DIM), jnp.bfloat16),
            pltpu.VMEM((640, HEAD_DIM), jnp.bfloat16),
            pltpu.VMEM((640, 2 * HEAD_DIM), jnp.bfloat16),
            pltpu.VMEM((PASSAGES, PASSAGE, HEAD_DIM), jnp.bfloat16),
            pltpu.VMEM((PASSAGES, PASSAGE, 2 * HEAD_DIM), jnp.bfloat16),
            pltpu.VMEM((PASSAGES, 8, PASSAGE), jnp.int32),
            pltpu.VMEM((heads * BLOCK, 2 * HEAD_DIM), jnp.float32),
        ],
        name="attend",
        cost_estimate=pl.CostEstimate(flops=2 * 10**9, bytes_accessed=5 * 10**6, transcendentals=0),
        compiler_params=pltpu.CompilerParams(vmem_limit_bytes=40 << 20),
    )(passage_ids, select_index, select_count, q_raw, kv_raw, inverse, select_index.reshape(ROWS, 1),
      table, old_table, incoming)


RELS = (1, 7, 2, 6, 3, 5, 4)
GROUPS = ((0, 2), (2, 2), (4, 3))
KV_PARTS = ((0, 48), (48, 32), (80, 32), (112, 32))
FLOWS = 4
SHARE = ROWS // FLOWS
STEPS = 7
MESH = pl.DeviceIdType.MESH


def exchange_kernel(
    ids_sm, pos_ref, hidden_ref, query_ref, keyvalue_ref, cache_ref,
    q_ref, kv_ref, inv_ref, table_ref, incoming_ref,
    held, weights, kv_weights, pool, outgoing, sending, arriving, partial, squares, fresh,
    local_sem, h_send, h_recv, z_send, z_recv, k_send, k_recv, kd_send, kd_recv,
    x_send, x_recv, f_send, f_recv, d_send, d_recv, r_send, r_recv,
    s_send, s_recv, g_send, g_recv, p_send, p_recv,
):
    store = lax.axis_index("store")
    rank = lax.axis_index("tp")
    x, high, core = store // 4, (store // 2) % 2, store % 2
    low, z = rank // 8, rank % 8
    quarter = z % 4
    head = rank // 4

    def place(to_x=x, to_core=core, to_low=low, to_z=z):
        return (to_x * 4 + high * 2 + to_core, to_low * 8 + to_z)

    def remote(source, target, send, recv, device):
        return pltpu.make_async_remote_copy(
            src_ref=source, dst_ref=target, send_sem=send, recv_sem=recv,
            device_id=device, device_id_type=MESH,
        )

    def piece(owner):
        return pl.ds(pl.multiple_of(owner * 64, 64), 64)

    locals_ = [
        pltpu.make_async_copy(hidden_ref, held.at[low], local_sem.at[0]),
        pltpu.make_async_copy(cache_ref.at[:, head], pool, local_sem.at[1]),
        pltpu.make_async_copy(query_ref.at[:, z], weights.at[7], local_sem.at[2]),
    ]
    for h in range(2):
        columns = pl.ds(pl.multiple_of((low * 2 + h) * 256, 256), 256)
        locals_.append(
            pltpu.make_async_copy(
                keyvalue_ref.at[:, columns], kv_weights.at[low, h], local_sem.at[3 + h]
            )
        )
    for copy in locals_:
        copy.start()

    barrier = pltpu.get_barrier_semaphore()
    for d in range(1, 16):
        pl.semaphore_signal(
            barrier, inc=1, device_id=((store + d) % 16, rank), device_id_type=MESH
        )
    for d in range(1, 8):
        pl.semaphore_signal(
            barrier, inc=1, device_id=place(to_z=(z + d) % 8), device_id_type=MESH
        )
    pl.semaphore_signal(barrier, inc=1, device_id=place(to_low=1 - low), device_id_type=MESH)
    pl.semaphore_wait(barrier, 23)

    across = place(to_low=1 - low)
    rows_of = [remote(
        hidden_ref.at[pl.ds(f * SHARE, SHARE)], held.at[low, pl.ds(f * SHARE, SHARE)],
        h_send.at[f], h_recv.at[f], across,
    ) for f in range(FLOWS)]
    mine = piece(x * 2 + core)
    spread = [remote(
        query_ref.at[:, (z + 8 - rel) % 8, mine], weights.at[o, :, mine],
        z_send.at[o], z_recv.at[o], place(to_z=(z + 8 - rel) % 8),
    ) for o, rel in enumerate(RELS)]
    half = pl.ds(pl.multiple_of(core * 256, 256), 256)
    kv_rows = []
    kv_shared = []
    for h in range(2):
        columns = pl.ds(pl.multiple_of(((1 - low) * 2 + h) * 256, 256), 256)
        kv_rows.append(remote(
            keyvalue_ref.at[half, columns], kv_weights.at[low, h, half],
            k_send.at[h], k_recv.at[h], across,
        ))
        kv_shared.append(remote(
            kv_weights.at[1 - low, h, half], kv_weights.at[1 - low, h, half],
            kd_send.at[h], kd_recv.at[h], place(to_core=1 - core),
        ))
    for copy in spread[:2] + rows_of + spread[2:] + kv_rows:
        copy.start()

    turn = 1 - 2 * core
    owners = (x, (x + 3) % 4, (x + 1) % 4, (x + 2) % 4)

    def group(g, owner):
        start, size = GROUPS[g]
        return weights.at[pl.ds(start, size), :, piece(owner * 2 + core)]

    def beside(g, way):
        to = (x + 1) % 4 if way == 0 else (x + 3) % 4
        return remote(
            group(g, x), group(g, x), x_send.at[g, way], x_recv.at[g, way], place(to_x=to)
        )

    def onward(g):
        owner = (x + 4 - turn) % 4
        to = (x + 4 + turn) % 4
        return remote(group(g, owner), group(g, owner), f_send.at[g], f_recv.at[g], place(to_x=to))

    def twin(g, i):
        block = group(g, owners[i])
        return remote(block, block, d_send.at[g, i], d_recv.at[g, i], place(to_core=1 - core))

    def first(g):
        start, size = GROUPS[g]
        for o in range(start, start + size):
            spread[o].wait_recv()
        beside(g, 0).start()
        beside(g, 1).start()
        twin(g, 0).start()

    def second(g):
        beside(g, 0).wait_recv()
        beside(g, 1).wait_recv()
        onward(g).start()
        twin(g, 1).start()
        twin(g, 2).start()

    def third(g):
        onward(g).wait_recv()
        twin(g, 3).start()

    def fourth(g):
        for i in range(4):
            twin(g, i).wait_recv()

    locals_[1].wait()

    def choose(d, carry):
        to = (store + d) % 16
        slot = jnp.int32(0)
        for k in range(PASSAGES):
            entry = ids_sm[to, k]
            slot = slot + jnp.where(entry // 4 == store, entry % 4, 0)
        outgoing[d] = pool[slot]
        return carry

    lax.fori_loop(0, 16, choose, 0)
    keep = pltpu.make_async_copy(outgoing.at[0], incoming_ref.at[store], local_sem.at[5])
    keep.start()
    passages = [remote(
        outgoing.at[d], incoming_ref.at[store], p_send.at[d - 1], p_recv.at[d - 1],
        ((store + d) % 16, rank),
    ) for d in range(1, 16)]

    first(0)
    first(1)
    second(0)
    first(2)
    third(0)
    second(1)
    third(1)
    second(2)
    for copy in passages:
        copy.start()
    for h in range(2):
        kv_rows[h].wait_recv()
        kv_shared[h].start()
    half_dim = HEAD_DIM // 2
    lane = lax.broadcasted_iota(jnp.int32, (1, HEAD_DIM), 1) % half_dim
    frequency = jnp.exp(lane.astype(jnp.float32) * (-2.0 * math.log(ROPE_BASE) / HEAD_DIM))
    angles = pos_ref[...].astype(jnp.float32) * frequency
    table_ref[:, :HEAD_DIM] = jnp.cos(angles)
    side = jnp.where(lax.broadcasted_iota(jnp.int32, (1, HEAD_DIM), 1) < half_dim, -1.0, 1.0)
    table_ref[:, HEAD_DIM:] = jnp.sin(angles) * side

    locals_[0].wait()
    locals_[2].wait()
    locals_[3].wait()
    locals_[4].wait()
    third(2)
    for h in range(2):
        kv_shared[h].wait_recv()
    fourth(0)
    fourth(1)
    fourth(2)

    def slot_of(f, s):
        if f % 2 == 0:
            return jnp.where(s < 3, 2 * s + 1, jnp.where(s == STEPS, 7, 12 - 2 * s))
        return jnp.where(s <= 3, 2 * s, jnp.where(s == STEPS, 7, 13 - 2 * s))

    def target_of(f, s):
        return (z + 15 - s) % 8 if f % 2 == 0 else (z + 1 + s) % 8

    def add_up(f, s):
        slot, to = slot_of(f, s), target_of(f, s)
        rows = pl.ds(f * SHARE, SHARE)
        offset, size = KV_PARTS[f]
        kv_rows_of = pl.ds(pl.multiple_of((to % 4) * SHARE + offset, 16), size)
        total = jnp.zeros((SHARE, 256), jnp.float32)
        kv_total = jnp.zeros((size, 256), jnp.float32)
        for b in range(2):
            total += jnp.dot(held[b, rows], weights[slot, b], preferred_element_type=jnp.float32)
            kv_total += jnp.dot(
                held[b, kv_rows_of], kv_weights[b, to // 4], preferred_element_type=jnp.float32
            )
        partial[f, :SHARE] = total
        partial[f, SHARE : SHARE + size] = kv_total

    def hop(f, s):
        to = (z + 1) % 8 if f % 2 == 0 else (z + 7) % 8
        size = SHARE + KV_PARTS[f][1]
        return remote(
            sending.at[f, s, pl.ds(0, size)], arriving.at[f, s, pl.ds(0, size)],
            r_send.at[f, s], r_recv.at[f, s], place(to_z=to),
        )

    for f in range(FLOWS):
        rows_of[f].wait_recv()
    for f in range(FLOWS):
        size = SHARE + KV_PARTS[f][1]
        add_up(f, 0)
        sending[f, 0, :size] = partial[f, :size].astype(jnp.bfloat16)
        hop(f, 0).start()

    ones = jnp.ones((8, 512), jnp.bfloat16)
    along = (((1,), (1,)), ((), ()))
    sum_of = jnp.zeros((8, ROWS), jnp.float32)
    for b in range(2):
        wide = held[b].astype(jnp.float32)
        square = wide * wide
        upper = square.astype(jnp.bfloat16)
        lower = (square - upper.astype(jnp.float32)).astype(jnp.bfloat16)
        sum_of += lax.dot_general(ones, upper, along, preferred_element_type=jnp.float32)
        sum_of += lax.dot_general(ones, lower, along, preferred_element_type=jnp.float32)
    squares[z, :, :ROWS] = sum_of
    squares[z, :, ROWS:] = jnp.zeros((8, 640 - ROWS), jnp.float32)
    sums = [remote(
        squares.at[z], squares.at[z], s_send.at[d - 1], s_recv.at[d - 1],
        place(to_z=(z + d) % 8),
    ) for d in range(1, 8)]
    for copy in sums:
        copy.start()

    def step(s, carry):
        for f in range(FLOWS):
            size = SHARE + KV_PARTS[f][1]
            add_up(f, s)
            hop(f, s - 1).wait_recv()
            total = partial[f, :size] + arriving[f, s - 1, :size].astype(jnp.float32)
            sending[f, s, :size] = total.astype(jnp.bfloat16)
            hop(f, s).start()
        return carry

    lax.fori_loop(1, STEPS, step, 0)
    for f in range(FLOWS):
        offset, size = KV_PARTS[f]
        add_up(f, jnp.int32(STEPS))
        hop(f, STEPS - 1).wait_recv()
        got = arriving[f, STEPS - 1].astype(jnp.float32)
        q_ref[f * SHARE : (f + 1) * SHARE] = partial[f, :SHARE] + got[:SHARE]
        kv_total = partial[f, SHARE : SHARE + size] + got[SHARE : SHARE + size]
        fresh[quarter, offset : offset + size] = kv_total.astype(jnp.bfloat16)
    shared = [remote(
        fresh.at[quarter], fresh.at[quarter], g_send.at[d - 1], g_recv.at[d - 1],
        place(to_z=(z // 4) * 4 + (quarter + d) % 4),
    ) for d in range(1, 4)]
    for copy in shared:
        copy.start()
    for copy in sums:
        copy.wait_recv()
    total = squares[0]
    for b in range(1, 8):
        total += squares[b]
    inv_ref[...] = jnp.transpose(lax.rsqrt(total * (1.0 / D) + EPSILON))
    for copy in shared:
        copy.wait_recv()
    for i in range(4):
        kv_ref[i * SHARE : (i + 1) * SHARE] = fresh[i]
    for copy in passages:
        copy.wait_recv()
    keep.wait()
    for copy in rows_of + spread + kv_rows + kv_shared + passages + sums + shared:
        copy.wait_send()
    for g in range(3):
        beside(g, 0).wait_send()
        beside(g, 1).wait_send()
        onward(g).wait_send()
        for i in range(4):
            twin(g, i).wait_send()

    def drained(s, carry):
        for f in range(FLOWS):
            hop(f, s).wait_send()
        return carry

    lax.fori_loop(0, STEPS, drained, 0)


def exchange(passage_ids, select_index, hidden, w_query, w_keyvalue, passage_cache):
    smem = pl.BlockSpec(memory_space=pltpu.SMEM)
    vmem = pl.BlockSpec(memory_space=pltpu.VMEM)
    hbm = pl.BlockSpec(memory_space=pl.ANY)
    dma = pltpu.SemaphoreType.DMA
    return pl.pallas_call(
        exchange_kernel,
        out_shape=(
            jax.ShapeDtypeStruct((ROWS, 256), jnp.float32),
            jax.ShapeDtypeStruct((ROWS, 256), jnp.bfloat16),
            jax.ShapeDtypeStruct((640, 8), jnp.float32),
            jax.ShapeDtypeStruct((ROWS, 2 * HEAD_DIM), jnp.float32),
            jax.ShapeDtypeStruct((16, PASSAGE, 256), jnp.bfloat16),
        ),
        in_specs=[smem, vmem, hbm, hbm, hbm, hbm],
        out_specs=(vmem, vmem, vmem, vmem, hbm),
        scratch_shapes=[
            pltpu.VMEM((2, ROWS, 512), jnp.bfloat16),
            pltpu.VMEM((8, 2, 512, 256), jnp.bfloat16),
            pltpu.VMEM((2, 2, 512, 256), jnp.bfloat16),
            pltpu.VMEM((4, PASSAGE, 256), jnp.bfloat16),
            pltpu.VMEM((16, PASSAGE, 256), jnp.bfloat16),
            pltpu.VMEM((FLOWS, STEPS, 192, 256), jnp.bfloat16),
            pltpu.VMEM((FLOWS, STEPS, 192, 256), jnp.bfloat16),
            pltpu.VMEM((FLOWS, 192, 256), jnp.float32),
            pltpu.VMEM((8, 8, 640), jnp.float32),
            pltpu.VMEM((4, SHARE, 256), jnp.bfloat16),
            dma((6,)), dma((4,)), dma((4,)), dma((7,)), dma((7,)), dma((2,)), dma((2,)),
            dma((2,)), dma((2,)), dma((3, 2)), dma((3, 2)), dma((3,)), dma((3,)),
            dma((3, 4)), dma((3, 4)), dma((4, 7)), dma((4, 7)), dma((7,)), dma((7,)),
            dma((3,)), dma((3,)), dma((15,)), dma((15,)),
        ],
        name="exchange",
        cost_estimate=pl.CostEstimate(
            flops=3 * 10**9, bytes_accessed=10**7, transcendentals=0
        ),
        compiler_params=pltpu.CompilerParams(
            collective_id=0, has_side_effects=True, vmem_limit_bytes=56 << 20
        ),
    )(
        passage_ids,
        select_index.reshape(ROWS, 1),
        hidden.reshape(ROWS, 512),
        w_query.reshape(2, 8, 512, 256),
        w_keyvalue,
        passage_cache,
    )


def local(hidden, w_query, w_keyvalue, passage_cache, passage_ids, select_index, select_count):
    q_raw, kv_raw, inverse, table, incoming = exchange(
        passage_ids, select_index, hidden, w_query, w_keyvalue, passage_cache
    )
    context = attend(
        passage_ids, select_index, select_count, q_raw, kv_raw, inverse, table, incoming
    )
    return context[None]


def solution(mesh):
    placed = (
        P("store", None, "tp"),
        P(None, "tp"),
        P("tp", None),
        P("store", None, None, None),
        P(),
        P("store", None),
        P("store"),
    )
    return jax.shard_map(
        local, mesh=mesh, in_specs=placed, out_specs=P("store", None, "tp"), check_vma=False
    )
```

```python
import math

import jax
import jax.numpy as jnp
from jax import lax
from jax.experimental import pallas as pl
from jax.experimental.pallas import tpu as pltpu
from jax.sharding import PartitionSpec as P

D = 8192
KV_HEADS = 4
HEAD_DIM = 128
PASSAGE = 384
PASSAGES = 8
SEQ = 3072
ROWS = 576
ROPE_BASE = 1000000.0
EPSILON = 1e-06
BLOCK = 192
SPAN = 2 * PASSAGE
NEG = -1e30
FAR = 1 << 20


def turned(vectors, cosine, sine):
    return vectors * cosine + pltpu.roll(vectors, HEAD_DIM // 2, 1) * sine


def turn_tables(positions):
    half = HEAD_DIM // 2
    frequency = ROPE_BASE ** (-(jnp.arange(half, dtype=jnp.float32) * 2.0) / HEAD_DIM)
    angles = positions.astype(jnp.float32)[..., None] * frequency
    cosine, sine = jnp.cos(angles), jnp.sin(angles)
    return jnp.concatenate([cosine, cosine, -sine, sine], axis=-1)


def attend_kernel(
    ids_sm, pos_sm, count_sm, q_hbm, kv_hbm, meta_hbm, table_hbm, old_table_ref, incoming_hbm,
    out_ref, q_in, kv_in, meta_ref, table_ref, old_ref, q_s, nk_s, nv_s, kk_s, vv_s, kp_s, acc_s,
    sem, old_sem,
):
    heads = q_in.shape[1] // HEAD_DIM
    store = lax.axis_index("store")
    fetched = [
        pltpu.make_async_copy(source, target, sem.at[i])
        for i, (source, target) in enumerate(
            ((meta_hbm, meta_ref), (kv_hbm, kv_in), (table_hbm, table_ref), (q_hbm, q_in))
        )
    ]
    fetched[0].start()
    olds = [
        pltpu.make_async_copy(incoming_hbm.at[ids_sm[store, k] // 4], old_ref.at[k], old_sem.at[k])
        for k in range(PASSAGES)
    ]
    for copy in olds + fetched[1:]:
        copy.start()
    count = count_sm[0]
    fetched[0].wait()
    inverse = meta_ref[:ROWS, :1]
    spot = meta_ref[:ROWS, 1:2].astype(jnp.int32)
    row_ids = lax.broadcasted_iota(jnp.int32, (ROWS, 1), 0)
    marked = jnp.where(row_ids < count, spot, -1)
    nv_s[:, HEAD_DIM:] = jnp.ones_like(nv_s[:, HEAD_DIM:])
    vv_s[:, HEAD_DIM:] = jnp.ones_like(vv_s[:, HEAD_DIM:])

    def mark(k, carry):
        here = k * PASSAGE + lax.broadcasted_iota(jnp.int32, (1, PASSAGE), 1)
        hit = jnp.max(jnp.where(marked == here, FAR, 0), axis=0, keepdims=True)
        kp_s[:, pl.ds(pl.multiple_of(k * PASSAGE, 128), PASSAGE)] = jnp.broadcast_to(
            jnp.maximum(here, hit), (8, PASSAGE)
        )
        return carry

    lax.fori_loop(0, PASSAGES, mark, 0)
    for k in range(PASSAGES):
        olds[k].wait()

    def prepare(k, carry):
        block = old_ref[k]
        table = old_table_ref[k]
        keys = block[:, :HEAD_DIM].astype(jnp.float32)
        rows = pl.ds(pl.multiple_of(k * PASSAGE, PASSAGE), PASSAGE)
        kk_s[rows] = turned(keys, table[:, :HEAD_DIM], table[:, HEAD_DIM:]).astype(jnp.bfloat16)
        vv_s[rows, :HEAD_DIM] = block[:, HEAD_DIM:]
        return carry

    lax.fori_loop(0, PASSAGES, prepare, 0)
    for copy in fetched[1:]:
        copy.wait()
    cosine, sine = table_ref[:, :HEAD_DIM], table_ref[:, HEAD_DIM:]
    scale = HEAD_DIM**-0.5 * math.log2(math.e)
    for h in range(heads):
        part = q_in[:, h * HEAD_DIM : (h + 1) * HEAD_DIM] * inverse
        q_s[h] = (turned(part, cosine, sine) * scale).astype(jnp.bfloat16)
    fresh = kv_in[:, :HEAD_DIM].astype(jnp.float32) * inverse
    nk_s[:ROWS] = turned(fresh, cosine, sine).astype(jnp.bfloat16)
    nk_s[ROWS:] = jnp.zeros_like(nk_s[ROWS:])
    nv_s[:ROWS, :HEAD_DIM] = (kv_in[:, HEAD_DIM:].astype(jnp.float32) * inverse).astype(jnp.bfloat16)
    nv_s[ROWS:, :HEAD_DIM] = jnp.zeros_like(nv_s[ROWS:, :HEAD_DIM])
    contract = (((1,), (1,)), ((), ()))
    for b in range(ROWS // BLOCK):
        low, high = b * BLOCK, (b + 1) * BLOCK
        rows = heads * BLOCK

        @pl.when(low >= count)
        def _():
            out_ref[low:high] = jnp.zeros_like(out_ref[low:high])

        @pl.when(low < count)
        def _():
            queries = q_s[:, low:high].reshape(rows, HEAD_DIM)
            width = -(-high // 128) * 128
            scores = lax.dot_general(
                queries, nk_s[:width], contract, preferred_element_type=jnp.float32
            )
            row_of = low + lax.broadcasted_iota(jnp.int32, (BLOCK, width), 0)
            key_of = lax.broadcasted_iota(jnp.int32, (BLOCK, width), 1)
            seen = jnp.concatenate([key_of <= row_of] * heads, axis=0)
            scores = jnp.where(seen, scores, NEG)
            top = jnp.max(scores, axis=1, keepdims=True)
            weight = jnp.exp2(scores - top).astype(jnp.bfloat16)
            acc_s[...] = jnp.dot(weight, nv_s[:width], preferred_element_type=jnp.float32)
            place = spot[low:high]
            place = jnp.concatenate([place] * heads, axis=0)
            last = jnp.minimum(count, high) - 1

            def old(i, top):
                span = pl.ds(pl.multiple_of(i * SPAN, SPAN), SPAN)
                scores = lax.dot_general(
                    queries, kk_s[span], contract, preferred_element_type=jnp.float32
                )
                scores = jnp.where(kp_s[0:1, span] <= place, scores, NEG)
                risen = jnp.maximum(top, jnp.max(scores, axis=1, keepdims=True))
                weight = jnp.exp2(scores - risen).astype(jnp.bfloat16)
                part = jnp.dot(weight, vv_s[span], preferred_element_type=jnp.float32)
                acc_s[...] = acc_s[...] * jnp.exp2(top - risen) + part
                return risen

            lax.fori_loop(0, pos_sm[0, last] // SPAN + 1, old, top)
            result = acc_s[:, :HEAD_DIM] / acc_s[:, HEAD_DIM:]
            live = low + lax.broadcasted_iota(jnp.int32, (BLOCK, HEAD_DIM), 0) < count
            for h in range(heads):
                piece = jnp.where(live, result[h * BLOCK : (h + 1) * BLOCK], 0.0)
                out_ref[low:high, h * HEAD_DIM : (h + 1) * HEAD_DIM] = piece.astype(jnp.bfloat16)


def attend(passage_ids, select_index, select_count, q_raw, kv_raw, meta, table, incoming):
    heads = q_raw.shape[1] // HEAD_DIM
    old_table = turn_tables(jnp.arange(PASSAGES) * PASSAGE)[:, None]
    smem = pl.BlockSpec(memory_space=pltpu.SMEM)
    vmem = pl.BlockSpec(memory_space=pltpu.VMEM)
    hbm = pl.BlockSpec(memory_space=pl.ANY)
    return pl.pallas_call(
        attend_kernel,
        out_shape=jax.ShapeDtypeStruct((ROWS, q_raw.shape[1]), jnp.bfloat16),
        in_specs=[smem] * 3 + [hbm] * 4 + [vmem, hbm],
        out_specs=vmem,
        scratch_shapes=[
            pltpu.VMEM(q_raw.shape, q_raw.dtype),
            pltpu.VMEM(kv_raw.shape, kv_raw.dtype),
            pltpu.VMEM(meta.shape, meta.dtype),
            pltpu.VMEM(table.shape, table.dtype),
            pltpu.VMEM((PASSAGES, PASSAGE, 2 * HEAD_DIM), jnp.bfloat16),
            pltpu.VMEM((heads, ROWS, HEAD_DIM), jnp.bfloat16),
            pltpu.VMEM((640, HEAD_DIM), jnp.bfloat16),
            pltpu.VMEM((640, 2 * HEAD_DIM), jnp.bfloat16),
            pltpu.VMEM((SEQ, HEAD_DIM), jnp.bfloat16),
            pltpu.VMEM((SEQ, 2 * HEAD_DIM), jnp.bfloat16),
            pltpu.VMEM((8, SEQ), jnp.int32),
            pltpu.VMEM((heads * BLOCK, 2 * HEAD_DIM), jnp.float32),
            pltpu.SemaphoreType.DMA((4,)),
            pltpu.SemaphoreType.DMA((PASSAGES,)),
        ],
        name="attend",
        cost_estimate=pl.CostEstimate(flops=2 * 10**9, bytes_accessed=5 * 10**6, transcendentals=0),
        compiler_params=pltpu.CompilerParams(vmem_limit_bytes=56 << 20),
    )(passage_ids, select_index, select_count, q_raw, kv_raw, meta, table, old_table, incoming)


RELS = (1, 7, 2, 6, 3, 5, 4)
SLOTS = (0, 1, 3, 4, 5, 6, 7)
KV_SLOT, OWN_SLOT = 2, 8
GROUPS = ((0, 3), (3, 2), (5, 2), (7, 1))
UP_SLOTS = (1, 4, 6, 7, 5, 3, 0, OWN_SLOT)
DOWN_SLOTS = (0, 3, 5, 7, 6, 4, 1, OWN_SLOT)
KV_PARTS = ((0, 48), (48, 32), (80, 32), (112, 32))
FLOWS = 4
ORDER = (0, 2, 1, 3)
ROUTES = ((1, 1), (3, 0), (2, 1), (1, 0), (3, 1), (2, 0), (0, 1))
SHARE = ROWS // FLOWS
STEPS = 7
MESH = pl.DeviceIdType.MESH


def exchange_kernel(
    ids_sm, pos_ref, hidden_ref, query_ref, keyvalue_ref, cache_ref,
    q_ref, kv_ref, meta_ref, table_ref, incoming_ref,
    held, weights, kv_own, pool, outgoing, sending, arriving, partial, squares, fresh, places,
    local_sem, h_send, h_recv, z_send, z_recv, k_send, k_recv,
    x_send, x_recv, f_send, f_recv, d_send, d_recv, r_send, r_recv,
    s_send, s_recv, g_send, g_recv, p_send, p_recv,
):
    store = lax.axis_index("store")
    rank = lax.axis_index("tp")
    x, high, core = store // 4, (store // 2) % 2, store % 2
    low, z = rank // 8, rank % 8
    quarter = z % 4
    head = rank // 4

    def place(to_x=x, to_core=core, to_low=low, to_z=z, to_high=high):
        return (to_x * 4 + to_high * 2 + to_core, to_low * 8 + to_z)

    def remote(source, target, send, recv, device):
        return pltpu.make_async_remote_copy(
            src_ref=source, dst_ref=target, send_sem=send, recv_sem=recv,
            device_id=device, device_id_type=MESH,
        )

    def piece(owner):
        return pl.ds(pl.multiple_of(owner * 64, 64), 64)

    locals_ = [
        pltpu.make_async_copy(hidden_ref, held.at[low], local_sem.at[0]),
        pltpu.make_async_copy(cache_ref.at[:, head], pool, local_sem.at[1]),
        pltpu.make_async_copy(query_ref.at[:, z], weights.at[OWN_SLOT], local_sem.at[2]),
    ]
    for h in range(2):
        columns = pl.ds(pl.multiple_of((low * 2 + h) * 256, 256), 256)
        locals_.append(
            pltpu.make_async_copy(
                keyvalue_ref.at[:, columns], kv_own.at[h], local_sem.at[3 + h]
            )
        )
    for copy in locals_:
        copy.start()

    barrier = pltpu.get_barrier_semaphore()
    for d in range(1, 16):
        pl.semaphore_signal(
            barrier, inc=1, device_id=((store + d) % 16, rank), device_id_type=MESH
        )
    for d in range(1, 8):
        pl.semaphore_signal(
            barrier, inc=1, device_id=place(to_z=(z + d) % 8), device_id_type=MESH
        )
    pl.semaphore_signal(barrier, inc=1, device_id=place(to_low=1 - low), device_id_type=MESH)
    pl.semaphore_wait(barrier, 23)

    across = place(to_low=1 - low)
    rows_of = remote(hidden_ref, held.at[low], h_send, h_recv, across)
    mine = piece(x * 2 + core)
    spread = [remote(
        query_ref.at[:, (z + 8 - rel) % 8, mine], weights.at[SLOTS[o], :, mine],
        z_send.at[o], z_recv.at[o], place(to_z=(z + 8 - rel) % 8),
    ) for o, rel in enumerate(RELS)]
    kv_rows = []
    for h in range(2):
        columns = pl.ds(pl.multiple_of(((1 - low) * 2 + h) * 256, 256), 256)
        kv_rows.append(remote(
            keyvalue_ref.at[mine, columns], weights.at[KV_SLOT, h, mine],
            k_send.at[h], k_recv.at[h], across,
        ))
    for copy in kv_rows + spread[:2] + [rows_of] + spread[2:]:
        copy.start()

    turn = 1 - 2 * core
    owners = (x, (x + 3) % 4, (x + 1) % 4, (x + 2) % 4)

    def group(g, owner):
        start, size = GROUPS[g]
        return weights.at[pl.ds(start, size), :, piece(owner * 2 + core)]

    def beside(g, way):
        to = (x + 1) % 4 if way == 0 else (x + 3) % 4
        return remote(
            group(g, x), group(g, x), x_send.at[g, way], x_recv.at[g, way], place(to_x=to)
        )

    def onward(g):
        owner = (x + 4 - turn) % 4
        to = (x + 4 + turn) % 4
        return remote(group(g, owner), group(g, owner), f_send.at[g], f_recv.at[g], place(to_x=to))

    def twin(g, i):
        block = group(g, owners[i])
        return remote(block, block, d_send.at[g, i], d_recv.at[g, i], place(to_core=1 - core))

    def first(g):
        for copy in (spread[:2] + kv_rows, spread[2:4], spread[4:6], spread[6:])[g]:
            copy.wait_recv()
        beside(g, 0).start()
        beside(g, 1).start()
        twin(g, 0).start()

    def second(g):
        beside(g, 0).wait_recv()
        beside(g, 1).wait_recv()
        onward(g).start()
        twin(g, 1).start()
        twin(g, 2).start()

    def third(g):
        onward(g).wait_recv()
        twin(g, 3).start()

    def fourth(g):
        for i in range(4):
            twin(g, i).wait_recv()

    locals_[1].wait()

    def choose(d, carry):
        to = (store + d) % 16
        slot = jnp.int32(0)
        for k in range(PASSAGES):
            entry = ids_sm[to, k]
            slot = slot + jnp.where(entry // 4 == store, entry % 4, 0)
        outgoing[d] = pool[slot]
        return carry

    lax.fori_loop(0, 16, choose, 0)
    places[...] = jnp.zeros_like(places)
    places[:, :ROWS] = jnp.broadcast_to(pos_ref[...].astype(jnp.float32), (8, ROWS))
    half_dim = HEAD_DIM // 2
    lane = lax.broadcasted_iota(jnp.int32, (1, HEAD_DIM), 1)
    frequency = jnp.exp(
        (lane % half_dim).astype(jnp.float32) * (-2.0 * math.log(ROPE_BASE) / HEAD_DIM)
    )
    angles = jnp.transpose(places[...])[:ROWS, :1] * frequency
    table_ref[:, :HEAD_DIM] = jnp.cos(angles)
    table_ref[:, HEAD_DIM:] = jnp.sin(angles) * jnp.where(lane < half_dim, -1.0, 1.0)
    keep = pltpu.make_async_copy(outgoing.at[0], incoming_ref.at[store], local_sem.at[5])
    keep.start()
    passages = []
    for other in range(2):
        for to_x, to_high in ROUTES + ((0, 0),) * other:
            to_x, to_high = (x + to_x) % 4, (high + to_high) % 2
            to = place(to_x=to_x, to_high=to_high, to_core=(core + other) % 2)
            i = len(passages)
            passages.append(remote(
                outgoing.at[(to[0] + 16 - store) % 16], incoming_ref.at[store],
                p_send.at[i], p_recv.at[i], to,
            ))

    first(0)
    first(1)
    second(0)
    first(2)
    second(1)
    first(3)
    third(0)
    second(2)
    fourth(0)
    locals_[0].wait()
    locals_[2].wait()
    locals_[3].wait()
    locals_[4].wait()
    rows_of.wait_recv()
    def slot_of(up, s):
        slots = UP_SLOTS if up else DOWN_SLOTS
        slot = slots[0]
        for i in range(1, STEPS + 1):
            slot = jnp.where(s == i, slots[i], slot)
        return slot

    def add_up(s):
        for way, rows, offset, size in ((0, 0, 0, 80), (1, 2 * SHARE, 80, 64)):
            slot = slot_of(way == 0, s)
            to = (z + 15 - s) % 8 if way == 0 else (z + 1 + s) % 8
            rows = pl.ds(rows, 2 * SHARE)
            kv_rows = pl.ds(pl.multiple_of((to % 4) * SHARE + offset, 16), size)
            total = jnp.zeros((2 * SHARE, 256), jnp.float32)
            for b in range(2):
                total += jnp.dot(held[b, rows], weights[slot, b], preferred_element_type=jnp.float32)
            partial[way, : 2 * SHARE] = total
            partial[way, 2 * SHARE : 2 * SHARE + size] = jnp.dot(
                held[low, kv_rows], kv_own[to // 4], preferred_element_type=jnp.float32
            ) + jnp.dot(
                held[1 - low, kv_rows],
                weights[KV_SLOT, to // 4],
                preferred_element_type=jnp.float32,
            )

    def parts_of(f):
        first_row = 2 * SHARE + (KV_PARTS[f][0] if f < 2 else KV_PARTS[f][0] - 80)
        return (
            partial[f // 2, f % 2 * SHARE : (f % 2 + 1) * SHARE],
            partial[f // 2, first_row : first_row + KV_PARTS[f][1]],
        )

    def hop(f, s):
        to = (z + 1) % 8 if f < 2 else (z + 7) % 8
        size = SHARE + KV_PARTS[f][1]
        return remote(
            sending.at[f, s, pl.ds(0, size)], arriving.at[f, s, pl.ds(0, size)],
            r_send.at[f, s], r_recv.at[f, s], place(to_z=to),
        )

    def forward(f, s, total, kv_total):
        sending[f, s, :SHARE] = total.astype(jnp.bfloat16)
        sending[f, s, SHARE : SHARE + KV_PARTS[f][1]] = kv_total.astype(jnp.bfloat16)
        hop(f, s).start()

    add_up(0)
    for f in ORDER:
        forward(f, 0, *parts_of(f))
    third(1)
    second(3)
    for copy in passages:
        copy.start()
    fourth(1)
    add_up(1)

    def relay(s):
        for f in ORDER:
            total, kv_total = parts_of(f)
            hop(f, s - 1).wait_recv()
            got = arriving[f, s - 1].astype(jnp.float32)
            size = SHARE + KV_PARTS[f][1]
            forward(f, s, total + got[:SHARE], kv_total + got[SHARE:size])

    relay(1)
    third(2)
    third(3)
    fourth(2)
    add_up(2)
    ones = jnp.ones((8, 512), jnp.bfloat16)
    along = (((1,), (1,)), ((), ()))
    sum_of = jnp.zeros((8, ROWS), jnp.float32)
    for b in range(2):
        wide = held[b].astype(jnp.float32)
        square = wide * wide
        upper = square.astype(jnp.bfloat16)
        lower = (square - upper.astype(jnp.float32)).astype(jnp.bfloat16)
        sum_of += lax.dot_general(ones, upper, along, preferred_element_type=jnp.float32)
        sum_of += lax.dot_general(ones, lower, along, preferred_element_type=jnp.float32)
    squares[z, :, :ROWS] = sum_of
    squares[z, :, ROWS:] = jnp.zeros((8, 640 - ROWS), jnp.float32)
    sums = [remote(
        squares.at[z], squares.at[z], s_send.at[d - 1], s_recv.at[d - 1],
        place(to_z=(z + d) % 8),
    ) for d in range(1, 8)]
    for copy in sums:
        copy.start()

    relay(2)
    fourth(3)
    add_up(3)

    def step(s, carry):
        relay(s)
        add_up(s + 1)
        return carry

    lax.fori_loop(3, STEPS, step, 0)
    for f in ORDER:
        offset, size = KV_PARTS[f]
        total, kv_total = parts_of(f)
        hop(f, STEPS - 1).wait_recv()
        got = arriving[f, STEPS - 1].astype(jnp.float32)
        q_ref[f * SHARE : (f + 1) * SHARE] = total + got[:SHARE]
        kv_total = kv_total + got[SHARE : SHARE + size]
        fresh[quarter, offset : offset + size] = kv_total.astype(jnp.bfloat16)
    shared = [remote(
        fresh.at[quarter], fresh.at[quarter], g_send.at[d - 1], g_recv.at[d - 1],
        place(to_z=(z // 4) * 4 + (quarter + d) % 4),
    ) for d in range(1, 4)]
    for copy in shared:
        copy.start()
    for copy in sums:
        copy.wait_recv()
    total = squares[0]
    for b in range(1, 8):
        total += squares[b]
    inverse = lax.rsqrt(total * (1.0 / D) + EPSILON)
    first_row = lax.broadcasted_iota(jnp.int32, (8, 640), 0) == 0
    meta_ref[...] = jnp.transpose(jnp.where(first_row, inverse, places[...]))
    for copy in shared:
        copy.wait_recv()
    for i in range(4):
        kv_ref[i * SHARE : (i + 1) * SHARE] = fresh[i]
    for copy in passages:
        copy.wait_recv()
    keep.wait()
    for copy in [rows_of] + spread + kv_rows + passages + sums + shared:
        copy.wait_send()
    for g in range(4):
        beside(g, 0).wait_send()
        beside(g, 1).wait_send()
        onward(g).wait_send()
        for i in range(4):
            twin(g, i).wait_send()

    def drained(s, carry):
        for f in range(FLOWS):
            hop(f, s).wait_send()
        return carry

    lax.fori_loop(0, STEPS, drained, 0)


def exchange(passage_ids, select_index, hidden, w_query, w_keyvalue, passage_cache):
    smem = pl.BlockSpec(memory_space=pltpu.SMEM)
    vmem = pl.BlockSpec(memory_space=pltpu.VMEM)
    hbm = pl.BlockSpec(memory_space=pltpu.HBM)
    dma = pltpu.SemaphoreType.DMA
    return pl.pallas_call(
        exchange_kernel,
        out_shape=(
            jax.ShapeDtypeStruct((ROWS, 256), jnp.float32),
            jax.ShapeDtypeStruct((ROWS, 256), jnp.bfloat16),
            jax.ShapeDtypeStruct((640, 8), jnp.float32),
            jax.ShapeDtypeStruct((ROWS, 2 * HEAD_DIM), jnp.float32),
            jax.ShapeDtypeStruct((16, PASSAGE, 256), jnp.bfloat16),
        ),
        in_specs=[smem, vmem, hbm, hbm, hbm, hbm],
        out_specs=(vmem, vmem, vmem, vmem, pl.BlockSpec(memory_space=pl.ANY)),
        scratch_shapes=[
            pltpu.VMEM((2, ROWS, 512), jnp.bfloat16),
            pltpu.VMEM((9, 2, 512, 256), jnp.bfloat16),
            pltpu.VMEM((2, 512, 256), jnp.bfloat16),
            pltpu.VMEM((4, PASSAGE, 256), jnp.bfloat16),
            pltpu.VMEM((16, PASSAGE, 256), jnp.bfloat16),
            pltpu.VMEM((FLOWS, STEPS, 192, 256), jnp.bfloat16),
            pltpu.VMEM((FLOWS, STEPS, 192, 256), jnp.bfloat16),
            pltpu.VMEM((2, 2 * SHARE + 80, 256), jnp.float32),
            pltpu.VMEM((8, 8, 640), jnp.float32),
            pltpu.VMEM((4, SHARE, 256), jnp.bfloat16),
            pltpu.VMEM((8, 640), jnp.float32),
            dma((6,)), dma(()), dma(()), dma((7,)), dma((7,)), dma((2,)), dma((2,)),
            dma((4, 2)), dma((4, 2)), dma((4,)), dma((4,)),
            dma((4, 4)), dma((4, 4)), dma((4, 7)), dma((4, 7)), dma((7,)), dma((7,)),
            dma((3,)), dma((3,)), dma((15,)), dma((15,)),
        ],
        name="exchange",
        cost_estimate=pl.CostEstimate(
            flops=3 * 10**9, bytes_accessed=10**7, transcendentals=0
        ),
        compiler_params=pltpu.CompilerParams(
            collective_id=0, has_side_effects=True, vmem_limit_bytes=56 << 20
        ),
    )(
        passage_ids,
        select_index,
        hidden.reshape(ROWS, 512),
        w_query.reshape(2, 8, 512, 256),
        w_keyvalue,
        passage_cache,
    )


def local(hidden, w_query, w_keyvalue, passage_cache, passage_ids, select_index, select_count):
    q_raw, kv_raw, meta, table, incoming = exchange(
        passage_ids, select_index, hidden, w_query, w_keyvalue, passage_cache
    )
    context = attend(
        passage_ids, select_index, select_count, q_raw, kv_raw, meta, table, incoming
    )
    return context[None]


def solution(mesh):
    placed = (
        P("store", None, "tp"),
        P(None, "tp"),
        P("tp", None),
        P("store", None, None, None),
        P(),
        P("store", None),
        P("store"),
    )
    return jax.shard_map(
        local, mesh=mesh, in_specs=placed, out_specs=P("store", None, "tp"), check_vma=False
    )
```

```python
import math

import jax
import jax.numpy as jnp
from jax import lax
from jax.experimental import pallas as pl
from jax.experimental.pallas import tpu as pltpu
from jax.sharding import PartitionSpec as P

D = 8192
KV_HEADS = 4
HEAD_DIM = 128
PASSAGE = 384
PASSAGES = 8
SEQ = 3072
ROWS = 576
ROPE_BASE = 1000000.0
EPSILON = 1e-06
BLOCK = 192
SPAN = 2 * PASSAGE
NEG = -1e30
CONTRACT = (((1,), (1,)), ((), ()))
FAR = 1 << 20


def turned(vectors, cosine, sine):
    return vectors * cosine + pltpu.roll(vectors, HEAD_DIM // 2, 1) * sine


def turn_tables(positions):
    half = HEAD_DIM // 2
    frequency = ROPE_BASE ** (-(jnp.arange(half, dtype=jnp.float32) * 2.0) / HEAD_DIM)
    angles = positions.astype(jnp.float32)[..., None] * frequency
    cosine, sine = jnp.cos(angles), jnp.sin(angles)
    return jnp.concatenate([cosine, cosine, -sine, sine], axis=-1)


def attend_kernel(
    slots_sm, pos_sm, count_sm, q_hbm, acc_hbm, marks_hbm, meta_hbm, old_table_ref, incoming_hbm,
    out_ref, q_s, acc_in, kp_s, meta_ref, old_ref, kk_s, vv_s, acc_s, sem, old_sem,
):
    heads = q_s.shape[0]
    olds = [
        pltpu.make_async_copy(incoming_hbm.at[slots_sm[0, k]], old_ref.at[k], old_sem.at[k])
        for k in range(PASSAGES)
    ]
    fetched = [
        pltpu.make_async_copy(source, target, sem.at[i])
        for i, (source, target) in enumerate(
            ((q_hbm, q_s), (acc_hbm, acc_in), (marks_hbm, kp_s), (meta_hbm, meta_ref))
        )
    ]
    for copy in olds + fetched:
        copy.start()
    count = count_sm[0]
    vv_s[:, HEAD_DIM:] = jnp.ones_like(vv_s[:, HEAD_DIM:])
    for k in range(PASSAGES):
        olds[k].wait()
        block = old_ref[k]
        table = old_table_ref[k]
        keys = block[:, :HEAD_DIM].astype(jnp.float32)
        rows = slice(k * PASSAGE, (k + 1) * PASSAGE)
        kk_s[rows] = turned(keys, table[:, :HEAD_DIM], table[:, HEAD_DIM:]).astype(jnp.bfloat16)
        vv_s[rows, :HEAD_DIM] = block[:, HEAD_DIM:]
    for copy in fetched:
        copy.wait()
    for b in range(ROWS // BLOCK):
        low, high = b * BLOCK, (b + 1) * BLOCK

        @pl.when(low >= count)
        def _():
            out_ref[low:high] = jnp.zeros_like(out_ref[low:high])

        @pl.when(low < count)
        def _():
            acc_s[...] = acc_in[b]
            tops = [acc_in[b, h * BLOCK : (h + 1) * BLOCK, 2 * HEAD_DIM - 1 :] for h in range(heads)]
            place = meta_ref[low:high, 1:2].astype(jnp.int32)
            last = jnp.minimum(count, high) - 1

            def old(i, tops):
                span = pl.ds(pl.multiple_of(i * SPAN, SPAN), SPAN)
                seen = kp_s[0:1, span] <= place
                raw = [
                    lax.dot_general(
                        q_s[h, low:high], kk_s[span], CONTRACT, preferred_element_type=jnp.float32
                    )
                    for h in range(heads)
                ]
                risen_tops = []
                for h, top in enumerate(tops):
                    mine = slice(h * BLOCK, (h + 1) * BLOCK)
                    scores = jnp.where(seen, raw[h], NEG)
                    risen = jnp.maximum(top, jnp.max(scores, axis=1, keepdims=True))
                    weight = jnp.exp2(scores - risen).astype(jnp.bfloat16)
                    part = jnp.dot(weight, vv_s[span], preferred_element_type=jnp.float32)
                    acc_s[mine] = acc_s[mine] * jnp.exp2(top - risen) + part
                    risen_tops.append(risen)
                return tuple(risen_tops)

            lax.fori_loop(0, pos_sm[0, last] // SPAN + 1, old, tuple(tops))
            result = acc_s[:, :HEAD_DIM] / acc_s[:, HEAD_DIM : HEAD_DIM + 1]
            live = low + lax.broadcasted_iota(jnp.int32, (BLOCK, HEAD_DIM), 0) < count
            for h in range(heads):
                piece = jnp.where(live, result[h * BLOCK : (h + 1) * BLOCK], 0.0)
                out_ref[low:high, h * HEAD_DIM : (h + 1) * HEAD_DIM] = piece.astype(jnp.bfloat16)


def attend(slots, select_index, select_count, queries, begun, marks, meta, incoming):
    heads = queries.shape[0]
    old_table = turn_tables(jnp.arange(PASSAGES) * PASSAGE)[:, None]
    smem = pl.BlockSpec(memory_space=pltpu.SMEM)
    vmem = pl.BlockSpec(memory_space=pltpu.VMEM)
    hbm = pl.BlockSpec(memory_space=pl.ANY)
    return pl.pallas_call(
        attend_kernel,
        out_shape=jax.ShapeDtypeStruct((ROWS, heads * HEAD_DIM), jnp.bfloat16),
        in_specs=[smem] * 3 + [hbm] * 4 + [vmem, hbm],
        out_specs=vmem,
        scratch_shapes=[
            pltpu.VMEM(queries.shape, queries.dtype),
            pltpu.VMEM(begun.shape, begun.dtype),
            pltpu.VMEM(marks.shape, marks.dtype),
            pltpu.VMEM(meta.shape, meta.dtype),
            pltpu.VMEM((PASSAGES, PASSAGE, 2 * HEAD_DIM), jnp.bfloat16),
            pltpu.VMEM((SEQ, HEAD_DIM), jnp.bfloat16),
            pltpu.VMEM((SEQ, 2 * HEAD_DIM), jnp.bfloat16),
            pltpu.VMEM((heads * BLOCK, 2 * HEAD_DIM), jnp.float32),
            pltpu.SemaphoreType.DMA((4,)),
            pltpu.SemaphoreType.DMA((PASSAGES,)),
        ],
        name="attend",
        cost_estimate=pl.CostEstimate(flops=2 * 10**9, bytes_accessed=5 * 10**6, transcendentals=0),
        compiler_params=pltpu.CompilerParams(vmem_limit_bytes=56 << 20),
    )(slots, select_index, select_count, queries, begun, marks, meta, old_table, incoming)


RELS = (1, 7, 2, 6, 3, 5, 4)
SLOTS = (0, 1, 3, 4, 5, 6, 7)
KV_SLOT, OWN_SLOT = 2, 8
GROUPS = ((0, 3), (3, 2), (5, 2), (7, 1))
UP_SLOTS = (1, 4, 6, 7, 5, 3, 0, OWN_SLOT)
DOWN_SLOTS = (0, 3, 5, 7, 6, 4, 1, OWN_SLOT)
QUERY_FLOWS = 4
FLOWS = 6
KV_PARTS = ((0, 80), (80, 64))
SIZES = (144, 144, 144, 144, 80, 64)
ORDER = (4, 5, 0, 2, 1, 3)
ROUTES = ((1, 1), (3, 0), (2, 1), (1, 0), (3, 1), (2, 0), (0, 1))
SHARE = ROWS // QUERY_FLOWS
STEPS = 7
MESH = pl.DeviceIdType.MESH


def exchange_kernel(
    ids_ref, count_sm, pos_ref, hidden_ref, query_ref, keyvalue_ref, cache_ref,
    queries_ref, begun_ref, marks_ref, meta_ref, slots_ref, incoming_ref,
    ids_sm, held, weights, kv_own, pool, outgoing, sending, arriving, partial, squares, fresh, places,
    q_raw, table_ref, nk_s, nv_s,
    local_sem, h_send, h_recv, z_send, z_recv, k_send, k_recv,
    x_send, x_recv, f_send, f_recv, d_send, d_recv, r_send, r_recv,
    s_send, s_recv, g_send, g_recv, p_send, p_recv,
):
    store = lax.axis_index("store")
    rank = lax.axis_index("tp")
    x, high, core = store // 4, (store // 2) % 2, store % 2
    low, z = rank // 8, rank % 8
    quarter = z % 4
    head = rank // 4

    def place(to_x=x, to_core=core, to_low=low, to_z=z, to_high=high):
        return (to_x * 4 + to_high * 2 + to_core, to_low * 8 + to_z)

    def remote(source, target, send, recv, device):
        return pltpu.make_async_remote_copy(
            src_ref=source, dst_ref=target, send_sem=send, recv_sem=recv,
            device_id=device, device_id_type=MESH,
        )

    def piece(owner):
        return pl.ds(pl.multiple_of(owner * 64, 64), 64)

    locals_ = [
        pltpu.make_async_copy(hidden_ref, held.at[low], local_sem.at[0]),
        pltpu.make_async_copy(cache_ref.at[:, head], pool, local_sem.at[1]),
        pltpu.make_async_copy(query_ref.at[:, z], weights.at[OWN_SLOT], local_sem.at[2]),
    ]
    for h in range(2):
        columns = pl.ds(pl.multiple_of((low * 2 + h) * 256, 256), 256)
        locals_.append(
            pltpu.make_async_copy(
                keyvalue_ref.at[:, columns], kv_own.at[h], local_sem.at[3 + h]
            )
        )
    locals_.append(pltpu.make_async_copy(ids_ref, ids_sm, local_sem.at[6]))
    for copy in locals_:
        copy.start()

    barrier = pltpu.get_barrier_semaphore()
    for d in range(1, 16):
        pl.semaphore_signal(
            barrier, inc=1, device_id=((store + d) % 16, rank), device_id_type=MESH
        )
    for d in range(1, 8):
        pl.semaphore_signal(
            barrier, inc=1, device_id=place(to_z=(z + d) % 8), device_id_type=MESH
        )
    pl.semaphore_signal(barrier, inc=1, device_id=place(to_low=1 - low), device_id_type=MESH)
    pl.semaphore_wait(barrier, 23)

    across = place(to_low=1 - low)
    rows_of = remote(hidden_ref, held.at[low], h_send, h_recv, across)
    mine = piece(x * 2 + core)
    spread = [remote(
        query_ref.at[:, (z + 8 - rel) % 8, mine], weights.at[SLOTS[o], :, mine],
        z_send.at[o], z_recv.at[o], place(to_z=(z + 8 - rel) % 8),
    ) for o, rel in enumerate(RELS)]
    kv_rows = []
    for h in range(2):
        columns = pl.ds(pl.multiple_of(((1 - low) * 2 + h) * 256, 256), 256)
        kv_rows.append(remote(
            keyvalue_ref.at[mine, columns], weights.at[KV_SLOT, h, mine],
            k_send.at[h], k_recv.at[h], across,
        ))
    for copy in kv_rows + spread[:2] + [rows_of] + spread[2:]:
        copy.start()

    turn = 1 - 2 * core
    owners = (x, (x + 3) % 4, (x + 1) % 4, (x + 2) % 4)

    def group(g, owner):
        start, size = GROUPS[g]
        return weights.at[pl.ds(start, size), :, piece(owner * 2 + core)]

    def beside(g, way):
        to = (x + 1) % 4 if way == 0 else (x + 3) % 4
        return remote(
            group(g, x), group(g, x), x_send.at[g, way], x_recv.at[g, way], place(to_x=to)
        )

    def onward(g):
        owner = (x + 4 - turn) % 4
        to = (x + 4 + turn) % 4
        return remote(group(g, owner), group(g, owner), f_send.at[g], f_recv.at[g], place(to_x=to))

    def twin(g, i):
        block = group(g, owners[i])
        return remote(block, block, d_send.at[g, i], d_recv.at[g, i], place(to_core=1 - core))

    def first(g):
        for copy in (spread[:2] + kv_rows, spread[2:4], spread[4:6], spread[6:])[g]:
            copy.wait_recv()
        beside(g, 0).start()
        beside(g, 1).start()
        twin(g, 0).start()

    def second(g):
        beside(g, 0).wait_recv()
        beside(g, 1).wait_recv()
        onward(g).start()
        twin(g, 1).start()
        twin(g, 2).start()

    def third(g):
        onward(g).wait_recv()
        twin(g, 3).start()

    def fourth(g):
        for i in range(4):
            twin(g, i).wait_recv()

    locals_[1].wait()
    locals_[5].wait()
    for k in range(PASSAGES):
        slots_ref[0, k] = ids_sm[k, store] // 4

    def choose(d, carry):
        to = (store + d) % 16
        slot = jnp.int32(0)
        for k in range(PASSAGES):
            entry = ids_sm[k, to]
            slot = slot + jnp.where(entry // 4 == store, entry % 4, 0)
        outgoing[d] = pool[slot]
        return carry

    lax.fori_loop(0, 16, choose, 0)
    places[...] = jnp.zeros_like(places)
    places[:, :ROWS] = jnp.broadcast_to(pos_ref[...].astype(jnp.float32), (8, ROWS))
    half_dim = HEAD_DIM // 2
    lane = lax.broadcasted_iota(jnp.int32, (1, HEAD_DIM), 1)
    frequency = jnp.exp(
        (lane % half_dim).astype(jnp.float32) * (-2.0 * math.log(ROPE_BASE) / HEAD_DIM)
    )
    spot = jnp.transpose(places[...])[:ROWS, :1]
    angles = spot * frequency
    row_ids = lax.broadcasted_iota(jnp.int32, (ROWS, 1), 0)
    marked = jnp.where(row_ids < count_sm[0], spot.astype(jnp.int32), -1)
    table_ref[:, :HEAD_DIM] = jnp.cos(angles)
    table_ref[:, HEAD_DIM:] = jnp.sin(angles) * jnp.where(lane < half_dim, -1.0, 1.0)
    for k in range(PASSAGES):
        here = k * PASSAGE + lax.broadcasted_iota(jnp.int32, (1, PASSAGE), 1)
        hit = jnp.max(jnp.where(marked == here, FAR, 0), axis=0, keepdims=True)
        marks_ref[:, k * PASSAGE : (k + 1) * PASSAGE] = jnp.broadcast_to(
            jnp.maximum(here, hit), (8, PASSAGE)
        )
    nv_s[:, HEAD_DIM:] = jnp.ones_like(nv_s[:, HEAD_DIM:])
    nk_s[ROWS:] = jnp.zeros_like(nk_s[ROWS:])
    nv_s[ROWS:, :HEAD_DIM] = jnp.zeros_like(nv_s[ROWS:, :HEAD_DIM])
    keep = pltpu.make_async_copy(outgoing.at[0], incoming_ref.at[store], local_sem.at[5])
    keep.start()
    passages = []
    for other in range(2):
        for to_x, to_high in ROUTES + ((0, 0),) * other:
            to_x, to_high = (x + to_x) % 4, (high + to_high) % 2
            to = place(to_x=to_x, to_high=to_high, to_core=(core + other) % 2)
            i = len(passages)
            passages.append(remote(
                outgoing.at[(to[0] + 16 - store) % 16], incoming_ref.at[store],
                p_send.at[i], p_recv.at[i], to,
            ))

    first(0)
    first(1)
    second(0)
    first(2)
    second(1)
    first(3)
    third(0)
    second(2)
    fourth(0)
    locals_[0].wait()
    locals_[2].wait()
    locals_[3].wait()
    locals_[4].wait()
    rows_of.wait_recv()
    def slot_of(up, s):
        slots = UP_SLOTS if up else DOWN_SLOTS
        slot = slots[0]
        for i in range(1, STEPS + 1):
            slot = jnp.where(s == i, slots[i], slot)
        return slot

    def add_up(s):
        for way, (offset, size) in enumerate(KV_PARTS):
            slot = slot_of(way == 0, s)
            to = (z + 15 - s) % 8 if way == 0 else (z + 1 + s) % 8
            rows = pl.ds(way * 2 * SHARE, 2 * SHARE)
            kv_rows = pl.ds(pl.multiple_of((to % 4) * SHARE + offset, 16), size)
            total = jnp.zeros((2 * SHARE, 256), jnp.float32)
            for b in range(2):
                total += jnp.dot(held[b, rows], weights[slot, b], preferred_element_type=jnp.float32)
            partial[way, : 2 * SHARE] = total
            partial[way, 2 * SHARE : 2 * SHARE + size] = jnp.dot(
                held[low, kv_rows], kv_own[to // 4], preferred_element_type=jnp.float32
            ) + jnp.dot(
                held[1 - low, kv_rows],
                weights[KV_SLOT, to // 4],
                preferred_element_type=jnp.float32,
            )

    def is_up(f):
        return f in (0, 1, 4)

    def part_of(f):
        if f < QUERY_FLOWS:
            return partial[f // 2, f % 2 * SHARE : (f % 2 + 1) * SHARE]
        return partial[f - QUERY_FLOWS, 2 * SHARE : 2 * SHARE + SIZES[f]]

    def hop(f, s):
        to = (z + 1) % 8 if is_up(f) else (z + 7) % 8
        rows = pl.ds(0, SIZES[f])
        return remote(
            sending.at[f, s, rows], arriving.at[f, s, rows],
            r_send.at[f, s], r_recv.at[f, s], place(to_z=to),
        )

    def forward(f, s, total):
        sending[f, s, : SIZES[f]] = total.astype(jnp.bfloat16)
        hop(f, s).start()

    add_up(0)
    for f in ORDER:
        forward(f, 0, part_of(f))
    third(1)
    second(3)
    for copy in passages:
        copy.start()
    fourth(1)
    add_up(1)

    def summed(f, s):
        hop(f, s).wait_recv()
        return part_of(f) + arriving[f, s, : SIZES[f]].astype(jnp.float32)

    def relay(s):
        for f in ORDER:
            forward(f, s, summed(f, s - 1))

    relay(1)
    third(2)
    third(3)
    fourth(2)
    add_up(2)
    ones = jnp.ones((8, 512), jnp.bfloat16)
    along = (((1,), (1,)), ((), ()))
    sum_of = jnp.zeros((8, ROWS), jnp.float32)
    for b in range(2):
        wide = held[b].astype(jnp.float32)
        square = wide * wide
        upper = square.astype(jnp.bfloat16)
        lower = (square - upper.astype(jnp.float32)).astype(jnp.bfloat16)
        sum_of += lax.dot_general(ones, upper, along, preferred_element_type=jnp.float32)
        sum_of += lax.dot_general(ones, lower, along, preferred_element_type=jnp.float32)
    squares[z, :, :ROWS] = sum_of
    squares[z, :, ROWS:] = jnp.zeros((8, 640 - ROWS), jnp.float32)
    sums = [remote(
        squares.at[z], squares.at[z], s_send.at[d - 1], s_recv.at[d - 1],
        place(to_z=(z + d) % 8),
    ) for d in range(1, 8)]
    for copy in sums:
        copy.start()

    relay(2)
    fourth(3)
    add_up(3)

    def step(s, carry):
        relay(s)
        add_up(s + 1)
        return carry

    lax.fori_loop(3, STEPS, step, 0)
    for f in range(QUERY_FLOWS, FLOWS):
        offset, size = KV_PARTS[f - QUERY_FLOWS]
        fresh[quarter, offset : offset + size] = summed(f, STEPS - 1).astype(jnp.bfloat16)
    shared = [remote(
        fresh.at[quarter], fresh.at[quarter], g_send.at[d - 1], g_recv.at[d - 1],
        place(to_z=(z // 4) * 4 + (quarter + d) % 4),
    ) for d in range(1, 4)]
    for copy in shared:
        copy.start()
    for f in ORDER[2:]:
        q_raw[f * SHARE : (f + 1) * SHARE] = summed(f, STEPS - 1)
    for copy in sums:
        copy.wait_recv()
    total = squares[0]
    for b in range(1, 8):
        total += squares[b]
    inverse = lax.rsqrt(total * (1.0 / D) + EPSILON)
    first_row = lax.broadcasted_iota(jnp.int32, (8, 640), 0) == 0
    meta = jnp.transpose(jnp.where(first_row, inverse, places[...]))
    meta_ref[...] = meta
    inverse = meta[:ROWS, :1]
    heads = q_raw.shape[1] // HEAD_DIM
    scale = HEAD_DIM**-0.5 * math.log2(math.e)
    for h in range(heads):
        part = q_raw[:, h * HEAD_DIM : (h + 1) * HEAD_DIM] * inverse
        part = turned(part, table_ref[:, :HEAD_DIM], table_ref[:, HEAD_DIM:])
        queries_ref[h] = (part * scale).astype(jnp.bfloat16)
    for copy in shared:
        copy.wait_recv()
    for i in range(4):
        rows = slice(i * SHARE, (i + 1) * SHARE)
        key_value = fresh[i].astype(jnp.float32) * inverse[rows]
        key = turned(key_value[:, :HEAD_DIM], table_ref[rows, :HEAD_DIM], table_ref[rows, HEAD_DIM:])
        nk_s[rows] = key.astype(jnp.bfloat16)
        nv_s[rows, :HEAD_DIM] = key_value[:, HEAD_DIM:].astype(jnp.bfloat16)
    for b in range(ROWS // BLOCK):
        begin, end = b * BLOCK, (b + 1) * BLOCK
        width = -(-end // 128) * 128
        queries = queries_ref[:, begin:end].reshape(heads * BLOCK, HEAD_DIM)
        scores = lax.dot_general(
            queries, nk_s[:width], CONTRACT, preferred_element_type=jnp.float32
        )
        row_of = begin + lax.broadcasted_iota(jnp.int32, (BLOCK, width), 0)
        key_of = lax.broadcasted_iota(jnp.int32, (BLOCK, width), 1)
        seen = jnp.concatenate([key_of <= row_of] * heads, axis=0)
        scores = jnp.where(seen, scores, NEG)
        top = jnp.max(scores, axis=1, keepdims=True)
        weight = jnp.exp2(scores - top).astype(jnp.bfloat16)
        acc = jnp.dot(weight, nv_s[:width], preferred_element_type=jnp.float32)
        last_lane = lax.broadcasted_iota(jnp.int32, acc.shape, 1) == 2 * HEAD_DIM - 1
        begun_ref[b] = jnp.where(last_lane, top, acc)
    for copy in passages:
        copy.wait_recv()
    keep.wait()
    for copy in [rows_of] + spread + kv_rows + passages + sums + shared:
        copy.wait_send()
    for g in range(4):
        beside(g, 0).wait_send()
        beside(g, 1).wait_send()
        onward(g).wait_send()
        for i in range(4):
            twin(g, i).wait_send()

    def drained(s, carry):
        for f in range(FLOWS):
            hop(f, s).wait_send()
        return carry

    lax.fori_loop(0, STEPS, drained, 0)


def exchange(passage_ids, select_count, select_index, hidden, w_query, w_keyvalue, passage_cache):
    smem = pl.BlockSpec(memory_space=pltpu.SMEM)
    vmem = pl.BlockSpec(memory_space=pltpu.VMEM)
    hbm = pl.BlockSpec(memory_space=pltpu.HBM)
    dma = pltpu.SemaphoreType.DMA
    return pl.pallas_call(
        exchange_kernel,
        out_shape=(
            jax.ShapeDtypeStruct((2, ROWS, HEAD_DIM), jnp.bfloat16),
            jax.ShapeDtypeStruct((ROWS // BLOCK, 2 * BLOCK, 256), jnp.float32),
            jax.ShapeDtypeStruct((8, SEQ), jnp.int32),
            jax.ShapeDtypeStruct((640, 8), jnp.float32),
            jax.ShapeDtypeStruct((1, PASSAGES), jnp.int32),
            jax.ShapeDtypeStruct((16, PASSAGE, 256), jnp.bfloat16),
        ),
        in_specs=[hbm, smem, vmem, hbm, hbm, hbm, hbm],
        out_specs=(vmem, vmem, vmem, vmem, smem, pl.BlockSpec(memory_space=pl.ANY)),
        scratch_shapes=[
            pltpu.SMEM((PASSAGES, 16), jnp.int32),
            pltpu.VMEM((2, ROWS, 512), jnp.bfloat16),
            pltpu.VMEM((9, 2, 512, 256), jnp.bfloat16),
            pltpu.VMEM((2, 512, 256), jnp.bfloat16),
            pltpu.VMEM((4, PASSAGE, 256), jnp.bfloat16),
            pltpu.VMEM((16, PASSAGE, 256), jnp.bfloat16),
            pltpu.VMEM((FLOWS, STEPS, SHARE, 256), jnp.bfloat16),
            pltpu.VMEM((FLOWS, STEPS, SHARE, 256), jnp.bfloat16),
            pltpu.VMEM((2, 2 * SHARE + 80, 256), jnp.float32),
            pltpu.VMEM((8, 8, 640), jnp.float32),
            pltpu.VMEM((4, SHARE, 256), jnp.bfloat16),
            pltpu.VMEM((8, 640), jnp.float32),
            pltpu.VMEM((ROWS, 256), jnp.float32),
            pltpu.VMEM((ROWS, 2 * HEAD_DIM), jnp.float32),
            pltpu.VMEM((640, HEAD_DIM), jnp.bfloat16),
            pltpu.VMEM((640, 2 * HEAD_DIM), jnp.bfloat16),
            dma((7,)), dma(()), dma(()), dma((7,)), dma((7,)), dma((2,)), dma((2,)),
            dma((4, 2)), dma((4, 2)), dma((4,)), dma((4,)),
            dma((4, 4)), dma((4, 4)), dma((6, 7)), dma((6, 7)), dma((7,)), dma((7,)),
            dma((3,)), dma((3,)), dma((15,)), dma((15,)),
        ],
        name="exchange",
        cost_estimate=pl.CostEstimate(
            flops=3 * 10**9, bytes_accessed=10**7, transcendentals=0
        ),
        compiler_params=pltpu.CompilerParams(
            collective_id=0, has_side_effects=True, vmem_limit_bytes=56 << 20
        ),
    )(
        passage_ids.T,
        select_count,
        select_index,
        hidden.reshape(ROWS, 512),
        w_query.reshape(2, 8, 512, 256),
        w_keyvalue,
        passage_cache,
    )


def local(hidden, w_query, w_keyvalue, passage_cache, passage_ids, select_index, select_count):
    queries, begun, marks, meta, slots, incoming = exchange(
        passage_ids, select_count, select_index, hidden, w_query, w_keyvalue, passage_cache
    )
    context = attend(
        slots, select_index, select_count, queries, begun, marks, meta, incoming
    )
    return context[None]


def solution(mesh):
    placed = (
        P("store", None, "tp"),
        P(None, "tp"),
        P("tp", None),
        P("store", None, None, None),
        P(),
        P("store", None),
        P("store"),
    )
    return jax.shard_map(
        local, mesh=mesh, in_specs=placed, out_specs=P("store", None, "tp"), check_vma=False
    )
```

```python
import math

import jax
import jax.numpy as jnp
from jax import lax
from jax.experimental import pallas as pl
from jax.experimental.pallas import tpu as pltpu
from jax.sharding import PartitionSpec as P

D = 8192
KV_HEADS = 4
HEAD_DIM = 128
PASSAGE = 384
PASSAGES = 8
SEQ = 3072
ROWS = 576
ROPE_BASE = 1000000.0
EPSILON = 1e-06
BLOCK = 192
SPAN = 2 * PASSAGE
NEG = -1e30
CONTRACT = (((1,), (1,)), ((), ()))
FAR = 1 << 20


def turned(vectors, cosine, sine):
    return vectors * cosine + pltpu.roll(vectors, HEAD_DIM // 2, 1) * sine


def turn_tables(positions):
    half = HEAD_DIM // 2
    frequency = ROPE_BASE ** (-(jnp.arange(half, dtype=jnp.float32) * 2.0) / HEAD_DIM)
    angles = positions.astype(jnp.float32)[..., None] * frequency
    cosine, sine = jnp.cos(angles), jnp.sin(angles)
    return jnp.concatenate([cosine, cosine, -sine, sine], axis=-1)


def attend_kernel(
    slots_sm, pos_sm, count_sm, q_hbm, acc_hbm, marks_hbm, meta_hbm, old_table_ref, incoming_hbm,
    out_ref, q_s, acc_in, kp_s, meta_ref, old_ref, kk_s, vv_s, acc_s, sem, old_sem,
):
    heads = q_s.shape[0]
    olds = [
        pltpu.make_async_copy(incoming_hbm.at[slots_sm[0, k]], old_ref.at[k], old_sem.at[k])
        for k in range(PASSAGES)
    ]
    fetched = [
        pltpu.make_async_copy(source, target, sem.at[i])
        for i, (source, target) in enumerate(
            ((q_hbm, q_s), (acc_hbm, acc_in), (marks_hbm, kp_s), (meta_hbm, meta_ref))
        )
    ]
    for copy in olds + fetched:
        copy.start()
    count = count_sm[0]
    vv_s[:, HEAD_DIM:] = jnp.ones_like(vv_s[:, HEAD_DIM:])
    for k in range(PASSAGES):
        olds[k].wait()
        block = old_ref[k]
        table = old_table_ref[k]
        keys = block[:, :HEAD_DIM].astype(jnp.float32)
        rows = slice(k * PASSAGE, (k + 1) * PASSAGE)
        kk_s[rows] = turned(keys, table[:, :HEAD_DIM], table[:, HEAD_DIM:]).astype(jnp.bfloat16)
        vv_s[rows, :HEAD_DIM] = block[:, HEAD_DIM:]
    for copy in fetched:
        copy.wait()
    for b in range(ROWS // BLOCK):
        low, high = b * BLOCK, (b + 1) * BLOCK

        @pl.when(low >= count)
        def _():
            out_ref[low:high] = jnp.zeros_like(out_ref[low:high])

        @pl.when(low < count)
        def _():
            acc_s[...] = acc_in[b]
            tops = [acc_in[b, h * BLOCK : (h + 1) * BLOCK, 2 * HEAD_DIM - 1 :] for h in range(heads)]
            place = meta_ref[low:high, 1:2].astype(jnp.int32)
            last = jnp.minimum(count, high) - 1

            def old(i, tops):
                span = pl.ds(pl.multiple_of(i * SPAN, SPAN), SPAN)
                seen = kp_s[0:1, span] <= place
                raw = [
                    lax.dot_general(
                        q_s[h, low:high], kk_s[span], CONTRACT, preferred_element_type=jnp.float32
                    )
                    for h in range(heads)
                ]
                risen_tops = []
                for h, top in enumerate(tops):
                    mine = slice(h * BLOCK, (h + 1) * BLOCK)
                    scores = jnp.where(seen, raw[h], NEG)
                    risen = jnp.maximum(top, jnp.max(scores, axis=1, keepdims=True))
                    weight = jnp.exp2(scores - risen).astype(jnp.bfloat16)
                    part = jnp.dot(weight, vv_s[span], preferred_element_type=jnp.float32)
                    acc_s[mine] = acc_s[mine] * jnp.exp2(top - risen) + part
                    risen_tops.append(risen)
                return tuple(risen_tops)

            lax.fori_loop(0, pos_sm[0, last] // SPAN + 1, old, tuple(tops))
            result = acc_s[:, :HEAD_DIM] / acc_s[:, HEAD_DIM : HEAD_DIM + 1]
            live = low + lax.broadcasted_iota(jnp.int32, (BLOCK, HEAD_DIM), 0) < count
            for h in range(heads):
                piece = jnp.where(live, result[h * BLOCK : (h + 1) * BLOCK], 0.0)
                out_ref[low:high, h * HEAD_DIM : (h + 1) * HEAD_DIM] = piece.astype(jnp.bfloat16)


def attend(slots, select_index, select_count, queries, begun, marks, meta, incoming):
    heads = queries.shape[0]
    old_table = turn_tables(jnp.arange(PASSAGES) * PASSAGE)[:, None]
    smem = pl.BlockSpec(memory_space=pltpu.SMEM)
    vmem = pl.BlockSpec(memory_space=pltpu.VMEM)
    hbm = pl.BlockSpec(memory_space=pl.ANY)
    return pl.pallas_call(
        attend_kernel,
        out_shape=jax.ShapeDtypeStruct((ROWS, heads * HEAD_DIM), jnp.bfloat16),
        in_specs=[smem] * 3 + [hbm] * 4 + [vmem, hbm],
        out_specs=vmem,
        scratch_shapes=[
            pltpu.VMEM(queries.shape, queries.dtype),
            pltpu.VMEM(begun.shape, begun.dtype),
            pltpu.VMEM(marks.shape, marks.dtype),
            pltpu.VMEM(meta.shape, meta.dtype),
            pltpu.VMEM((PASSAGES, PASSAGE, 2 * HEAD_DIM), jnp.bfloat16),
            pltpu.VMEM((SEQ, HEAD_DIM), jnp.bfloat16),
            pltpu.VMEM((SEQ, 2 * HEAD_DIM), jnp.bfloat16),
            pltpu.VMEM((heads * BLOCK, 2 * HEAD_DIM), jnp.float32),
            pltpu.SemaphoreType.DMA((4,)),
            pltpu.SemaphoreType.DMA((PASSAGES,)),
        ],
        name="attend",
        cost_estimate=pl.CostEstimate(flops=2 * 10**9, bytes_accessed=5 * 10**6, transcendentals=0),
        compiler_params=pltpu.CompilerParams(vmem_limit_bytes=56 << 20),
    )(slots, select_index, select_count, queries, begun, marks, meta, old_table, incoming)


RELS = (1, 7, 2, 6, 3, 5, 4)
SLOTS = (0, 1, 3, 4, 5, 6, 7)
KV_SLOT, OWN_SLOT = 2, 8
GROUPS = ((0, 3), (3, 2), (5, 2), (7, 1))
UP_SLOTS = (1, 4, 6, 7, 5, 3, 0, OWN_SLOT)
DOWN_SLOTS = (0, 3, 5, 7, 6, 4, 1, OWN_SLOT)
QUERY_FLOWS = 4
FLOWS = 6
KV_PARTS = ((0, 80), (80, 64))
SIZES = (144, 144, 144, 144, 80, 64)
ORDER = (0, 2, 1, 3)
KV_ORDER = (4, 5)
ROUTES = ((1, 1), (3, 0), (2, 1), (1, 0), (3, 1), (2, 0), (0, 1))
SHARE = ROWS // QUERY_FLOWS
STEPS = 7
MESH = pl.DeviceIdType.MESH


def exchange_kernel(
    ids_ref, count_sm, pos_ref, hidden_ref, query_ref, keyvalue_ref, cache_ref,
    queries_ref, begun_ref, marks_ref, meta_ref, slots_ref, incoming_ref,
    ids_sm, held, weights, kv_own, pool, outgoing, sending, arriving, partial, kv_partial, squares, fresh, places,
    q_raw, table_ref, nk_s, nv_s,
    local_sem, h_send, h_recv, z_send, z_recv, k_send, k_recv,
    x_send, x_recv, f_send, f_recv, d_send, d_recv, r_send, r_recv,
    s_send, s_recv, g_send, g_recv, p_send, p_recv,
):
    store = lax.axis_index("store")
    rank = lax.axis_index("tp")
    x, high, core = store // 4, (store // 2) % 2, store % 2
    low, z = rank // 8, rank % 8
    quarter = z % 4
    head = rank // 4

    def place(to_x=x, to_core=core, to_low=low, to_z=z, to_high=high):
        return (to_x * 4 + to_high * 2 + to_core, to_low * 8 + to_z)

    def remote(source, target, send, recv, device):
        return pltpu.make_async_remote_copy(
            src_ref=source, dst_ref=target, send_sem=send, recv_sem=recv,
            device_id=device, device_id_type=MESH,
        )

    def piece(owner):
        return pl.ds(pl.multiple_of(owner * 64, 64), 64)

    locals_ = [
        pltpu.make_async_copy(hidden_ref, held.at[low], local_sem.at[0]),
        pltpu.make_async_copy(cache_ref.at[:, head], pool, local_sem.at[1]),
        pltpu.make_async_copy(query_ref.at[:, z], weights.at[OWN_SLOT], local_sem.at[2]),
    ]
    for h in range(2):
        columns = pl.ds(pl.multiple_of((low * 2 + h) * 256, 256), 256)
        locals_.append(
            pltpu.make_async_copy(
                keyvalue_ref.at[:, columns], kv_own.at[h], local_sem.at[3 + h]
            )
        )
    locals_.append(pltpu.make_async_copy(ids_ref, ids_sm, local_sem.at[6]))
    for copy in locals_:
        copy.start()

    barrier = pltpu.get_barrier_semaphore()
    for d in range(1, 16):
        pl.semaphore_signal(
            barrier, inc=1, device_id=((store + d) % 16, rank), device_id_type=MESH
        )
    for d in range(1, 8):
        pl.semaphore_signal(
            barrier, inc=1, device_id=place(to_z=(z + d) % 8), device_id_type=MESH
        )
    pl.semaphore_signal(barrier, inc=1, device_id=place(to_low=1 - low), device_id_type=MESH)
    pl.semaphore_wait(barrier, 23)

    across = place(to_low=1 - low)
    rows_of = remote(hidden_ref, held.at[low], h_send, h_recv, across)
    mine = piece(x * 2 + core)
    spread = [remote(
        query_ref.at[:, (z + 8 - rel) % 8, mine], weights.at[SLOTS[o], :, mine],
        z_send.at[o], z_recv.at[o], place(to_z=(z + 8 - rel) % 8),
    ) for o, rel in enumerate(RELS)]
    kv_rows = []
    for h in range(2):
        columns = pl.ds(pl.multiple_of(((1 - low) * 2 + h) * 256, 256), 256)
        kv_rows.append(remote(
            keyvalue_ref.at[mine, columns], weights.at[KV_SLOT, h, mine],
            k_send.at[h], k_recv.at[h], across,
        ))
    for copy in kv_rows + spread[:2] + [rows_of] + spread[2:]:
        copy.start()

    turn = 1 - 2 * core
    owners = (x, (x + 3) % 4, (x + 1) % 4, (x + 2) % 4)

    def group(g, owner):
        start, size = GROUPS[g]
        return weights.at[pl.ds(start, size), :, piece(owner * 2 + core)]

    def beside(g, way):
        to = (x + 1) % 4 if way == 0 else (x + 3) % 4
        return remote(
            group(g, x), group(g, x), x_send.at[g, way], x_recv.at[g, way], place(to_x=to)
        )

    def onward(g):
        owner = (x + 4 - turn) % 4
        to = (x + 4 + turn) % 4
        return remote(group(g, owner), group(g, owner), f_send.at[g], f_recv.at[g], place(to_x=to))

    def twin(g, i):
        block = group(g, owners[i])
        return remote(block, block, d_send.at[g, i], d_recv.at[g, i], place(to_core=1 - core))

    def first(g):
        for copy in (spread[:2] + kv_rows, spread[2:4], spread[4:6], spread[6:])[g]:
            copy.wait_recv()
        beside(g, 0).start()
        beside(g, 1).start()
        twin(g, 0).start()

    def second(g):
        beside(g, 0).wait_recv()
        beside(g, 1).wait_recv()
        onward(g).start()
        twin(g, 1).start()
        twin(g, 2).start()

    def third(g):
        onward(g).wait_recv()
        twin(g, 3).start()

    def fourth(g):
        for i in range(4):
            twin(g, i).wait_recv()

    locals_[1].wait()
    locals_[5].wait()
    for k in range(PASSAGES):
        slots_ref[0, k] = ids_sm[k, store] // 4

    def choose(d, carry):
        to = (store + d) % 16
        slot = jnp.int32(0)
        for k in range(PASSAGES):
            entry = ids_sm[k, to]
            slot = slot + jnp.where(entry // 4 == store, entry % 4, 0)
        outgoing[d] = pool[slot]
        return carry

    lax.fori_loop(0, 16, choose, 0)
    places[...] = jnp.zeros_like(places)
    places[:, :ROWS] = jnp.broadcast_to(pos_ref[...].astype(jnp.float32), (8, ROWS))
    half_dim = HEAD_DIM // 2
    lane = lax.broadcasted_iota(jnp.int32, (1, HEAD_DIM), 1)
    frequency = jnp.exp(
        (lane % half_dim).astype(jnp.float32) * (-2.0 * math.log(ROPE_BASE) / HEAD_DIM)
    )
    spot = jnp.transpose(places[...])[:ROWS, :1]
    angles = spot * frequency
    row_ids = lax.broadcasted_iota(jnp.int32, (ROWS, 1), 0)
    marked = jnp.where(row_ids < count_sm[0], spot.astype(jnp.int32), -1)
    table_ref[:, :HEAD_DIM] = jnp.cos(angles)
    table_ref[:, HEAD_DIM:] = jnp.sin(angles) * jnp.where(lane < half_dim, -1.0, 1.0)
    for k in range(PASSAGES):
        here = k * PASSAGE + lax.broadcasted_iota(jnp.int32, (1, PASSAGE), 1)
        hit = jnp.max(jnp.where(marked == here, FAR, 0), axis=0, keepdims=True)
        marks_ref[:, k * PASSAGE : (k + 1) * PASSAGE] = jnp.broadcast_to(
            jnp.maximum(here, hit), (8, PASSAGE)
        )
    nv_s[:, HEAD_DIM:] = jnp.ones_like(nv_s[:, HEAD_DIM:])
    nk_s[ROWS:] = jnp.zeros_like(nk_s[ROWS:])
    nv_s[ROWS:, :HEAD_DIM] = jnp.zeros_like(nv_s[ROWS:, :HEAD_DIM])
    keep = pltpu.make_async_copy(outgoing.at[0], incoming_ref.at[store], local_sem.at[5])
    keep.start()
    passages = []
    for other in range(2):
        for to_x, to_high in ROUTES + ((0, 0),) * other:
            to_x, to_high = (x + to_x) % 4, (high + to_high) % 2
            to = place(to_x=to_x, to_high=to_high, to_core=(core + other) % 2)
            i = len(passages)
            passages.append(remote(
                outgoing.at[(to[0] + 16 - store) % 16], incoming_ref.at[store],
                p_send.at[i], p_recv.at[i], to,
            ))

    first(0)
    first(1)
    second(0)
    first(2)
    second(1)
    first(3)
    third(0)
    second(2)
    fourth(0)
    locals_[0].wait()
    locals_[2].wait()
    locals_[3].wait()
    locals_[4].wait()
    rows_of.wait_recv()
    def slot_of(up, s):
        slots = UP_SLOTS if up else DOWN_SLOTS
        slot = slots[0]
        for i in range(1, STEPS + 1):
            slot = jnp.where(s == i, slots[i], slot)
        return slot

    def add_up(s):
        for way in range(2):
            slot = slot_of(way == 0, s)
            rows = pl.ds(way * 2 * SHARE, 2 * SHARE)
            total = jnp.zeros((2 * SHARE, 256), jnp.float32)
            for b in range(2):
                total += jnp.dot(held[b, rows], weights[slot, b], preferred_element_type=jnp.float32)
            partial[way] = total

    def add_up_kv(s, carry):
        for way, (offset, size) in enumerate(KV_PARTS):
            to = (z + 15 - s) % 8 if way == 0 else (z + 1 + s) % 8
            kv_rows = pl.ds(pl.multiple_of((to % 4) * SHARE + offset, 16), size)
            kv_partial[s, offset : offset + size] = jnp.dot(
                held[low, kv_rows], kv_own[to // 4], preferred_element_type=jnp.float32
            ) + jnp.dot(
                held[1 - low, kv_rows],
                weights[KV_SLOT, to // 4],
                preferred_element_type=jnp.float32,
            )
        return carry

    def is_up(f):
        return f in (0, 1, 4)

    def part_of(f, s):
        if f < QUERY_FLOWS:
            return partial[f // 2, f % 2 * SHARE : (f % 2 + 1) * SHARE]
        offset, size = KV_PARTS[f - QUERY_FLOWS]
        return kv_partial[s, offset : offset + size]

    def hop(f, s):
        to = (z + 1) % 8 if is_up(f) else (z + 7) % 8
        rows = pl.ds(0, SIZES[f])
        return remote(
            sending.at[f, s, rows], arriving.at[f, s, rows],
            r_send.at[f, s], r_recv.at[f, s], place(to_z=to),
        )

    def forward(f, s, total):
        sending[f, s, : SIZES[f]] = total.astype(jnp.bfloat16)
        hop(f, s).start()

    def summed(f, s):
        hop(f, s).wait_recv()
        return part_of(f, s + 1) + arriving[f, s, : SIZES[f]].astype(jnp.float32)

    def relay(s, flows=ORDER):
        for f in flows:
            forward(f, s, summed(f, s - 1))

    add_up_kv(0, 0)
    for f in KV_ORDER:
        forward(f, 0, part_of(f, 0))
    add_up(0)
    for f in ORDER:
        forward(f, 0, part_of(f, 0))
    third(1)
    lax.fori_loop(1, STEPS + 1, add_up_kv, 0)
    relay(1, KV_ORDER)
    second(3)
    for copy in passages:
        copy.start()
    fourth(1)
    add_up(1)

    relay(2, KV_ORDER)
    relay(1)
    third(2)
    third(3)
    fourth(2)
    add_up(2)
    ones = jnp.ones((8, 512), jnp.bfloat16)
    along = (((1,), (1,)), ((), ()))
    sum_of = jnp.zeros((8, ROWS), jnp.float32)
    for b in range(2):
        wide = held[b].astype(jnp.float32)
        square = wide * wide
        upper = square.astype(jnp.bfloat16)
        lower = (square - upper.astype(jnp.float32)).astype(jnp.bfloat16)
        sum_of += lax.dot_general(ones, upper, along, preferred_element_type=jnp.float32)
        sum_of += lax.dot_general(ones, lower, along, preferred_element_type=jnp.float32)
    squares[z, :, :ROWS] = sum_of
    squares[z, :, ROWS:] = jnp.zeros((8, 640 - ROWS), jnp.float32)
    sums = [remote(
        squares.at[z], squares.at[z], s_send.at[d - 1], s_recv.at[d - 1],
        place(to_z=(z + d) % 8),
    ) for d in range(1, 8)]
    for copy in sums:
        copy.start()

    relay(3, KV_ORDER)
    relay(2)
    fourth(3)
    add_up(3)
    relay(4, KV_ORDER)
    relay(3)
    add_up(4)
    relay(5, KV_ORDER)
    relay(4)
    add_up(5)
    relay(6, KV_ORDER)
    relay(5)
    add_up(6)
    for f in range(QUERY_FLOWS, FLOWS):
        offset, size = KV_PARTS[f - QUERY_FLOWS]
        fresh[quarter, offset : offset + size] = summed(f, STEPS - 1).astype(jnp.bfloat16)
    shared = [remote(
        fresh.at[quarter], fresh.at[quarter], g_send.at[d - 1], g_recv.at[d - 1],
        place(to_z=(z // 4) * 4 + (quarter + d) % 4),
    ) for d in range(1, 4)]
    for copy in shared:
        copy.start()
    relay(6)
    add_up(STEPS)
    heads = q_raw.shape[1] // HEAD_DIM
    scale = HEAD_DIM**-0.5 * math.log2(math.e)
    for copy in sums:
        copy.wait_recv()
    total = squares[0]
    for b in range(1, 8):
        total += squares[b]
    inverse = lax.rsqrt(total * (1.0 / D) + EPSILON)
    first_row = lax.broadcasted_iota(jnp.int32, (8, 640), 0) == 0
    meta = jnp.transpose(jnp.where(first_row, inverse, places[...]))
    meta_ref[...] = meta
    inverse = meta[:ROWS, :1]
    for copy in shared:
        copy.wait_recv()
    for i in range(4):
        rows = slice(i * SHARE, (i + 1) * SHARE)
        key_value = fresh[i].astype(jnp.float32) * inverse[rows]
        key = turned(key_value[:, :HEAD_DIM], table_ref[rows, :HEAD_DIM], table_ref[rows, HEAD_DIM:])
        nk_s[rows] = key.astype(jnp.bfloat16)
        nv_s[rows, :HEAD_DIM] = key_value[:, HEAD_DIM:].astype(jnp.bfloat16)
    for f in ORDER:
        q_raw[f * SHARE : (f + 1) * SHARE] = summed(f, STEPS - 1)
    for h in range(heads):
        part = q_raw[:, h * HEAD_DIM : (h + 1) * HEAD_DIM] * inverse
        part = turned(part, table_ref[:, :HEAD_DIM], table_ref[:, HEAD_DIM:])
        queries_ref[h] = (part * scale).astype(jnp.bfloat16)
    for b in range(ROWS // BLOCK):
        begin, end = b * BLOCK, (b + 1) * BLOCK
        width = -(-end // 128) * 128
        queries = queries_ref[:, begin:end].reshape(heads * BLOCK, HEAD_DIM)
        scores = lax.dot_general(
            queries, nk_s[:width], CONTRACT, preferred_element_type=jnp.float32
        )
        row_of = begin + lax.broadcasted_iota(jnp.int32, (BLOCK, width), 0)
        key_of = lax.broadcasted_iota(jnp.int32, (BLOCK, width), 1)
        seen = jnp.concatenate([key_of <= row_of] * heads, axis=0)
        scores = jnp.where(seen, scores, NEG)
        top = jnp.max(scores, axis=1, keepdims=True)
        weight = jnp.exp2(scores - top).astype(jnp.bfloat16)
        acc = jnp.dot(weight, nv_s[:width], preferred_element_type=jnp.float32)
        last_lane = lax.broadcasted_iota(jnp.int32, acc.shape, 1) == 2 * HEAD_DIM - 1
        begun_ref[b] = jnp.where(last_lane, top, acc)
    for copy in passages:
        copy.wait_recv()
    keep.wait()
    for copy in [rows_of] + spread + kv_rows + passages + sums + shared:
        copy.wait_send()
    for g in range(4):
        beside(g, 0).wait_send()
        beside(g, 1).wait_send()
        onward(g).wait_send()
        for i in range(4):
            twin(g, i).wait_send()

    def drained(s, carry):
        for f in range(FLOWS):
            hop(f, s).wait_send()
        return carry

    lax.fori_loop(0, STEPS, drained, 0)


def exchange(passage_ids, select_count, select_index, hidden, w_query, w_keyvalue, passage_cache):
    smem = pl.BlockSpec(memory_space=pltpu.SMEM)
    vmem = pl.BlockSpec(memory_space=pltpu.VMEM)
    hbm = pl.BlockSpec(memory_space=pltpu.HBM)
    dma = pltpu.SemaphoreType.DMA
    return pl.pallas_call(
        exchange_kernel,
        out_shape=(
            jax.ShapeDtypeStruct((2, ROWS, HEAD_DIM), jnp.bfloat16),
            jax.ShapeDtypeStruct((ROWS // BLOCK, 2 * BLOCK, 256), jnp.float32),
            jax.ShapeDtypeStruct((8, SEQ), jnp.int32),
            jax.ShapeDtypeStruct((640, 8), jnp.float32),
            jax.ShapeDtypeStruct((1, PASSAGES), jnp.int32),
            jax.ShapeDtypeStruct((16, PASSAGE, 256), jnp.bfloat16),
        ),
        in_specs=[hbm, smem, vmem, hbm, hbm, hbm, hbm],
        out_specs=(vmem, vmem, vmem, vmem, smem, pl.BlockSpec(memory_space=pl.ANY)),
        scratch_shapes=[
            pltpu.SMEM((PASSAGES, 16), jnp.int32),
            pltpu.VMEM((2, ROWS, 512), jnp.bfloat16),
            pltpu.VMEM((9, 2, 512, 256), jnp.bfloat16),
            pltpu.VMEM((2, 512, 256), jnp.bfloat16),
            pltpu.VMEM((4, PASSAGE, 256), jnp.bfloat16),
            pltpu.VMEM((16, PASSAGE, 256), jnp.bfloat16),
            pltpu.VMEM((FLOWS, STEPS, SHARE, 256), jnp.bfloat16),
            pltpu.VMEM((FLOWS, STEPS, SHARE, 256), jnp.bfloat16),
            pltpu.VMEM((2, 2 * SHARE, 256), jnp.float32),
            pltpu.VMEM((STEPS + 1, SHARE, 256), jnp.float32),
            pltpu.VMEM((8, 8, 640), jnp.float32),
            pltpu.VMEM((4, SHARE, 256), jnp.bfloat16),
            pltpu.VMEM((8, 640), jnp.float32),
            pltpu.VMEM((ROWS, 256), jnp.float32),
            pltpu.VMEM((ROWS, 2 * HEAD_DIM), jnp.float32),
            pltpu.VMEM((640, HEAD_DIM), jnp.bfloat16),
            pltpu.VMEM((640, 2 * HEAD_DIM), jnp.bfloat16),
            dma((7,)), dma(()), dma(()), dma((7,)), dma((7,)), dma((2,)), dma((2,)),
            dma((4, 2)), dma((4, 2)), dma((4,)), dma((4,)),
            dma((4, 4)), dma((4, 4)), dma((6, 7)), dma((6, 7)), dma((7,)), dma((7,)),
            dma((3,)), dma((3,)), dma((15,)), dma((15,)),
        ],
        name="exchange",
        cost_estimate=pl.CostEstimate(
            flops=3 * 10**9, bytes_accessed=10**7, transcendentals=0
        ),
        compiler_params=pltpu.CompilerParams(
            collective_id=0, has_side_effects=True, vmem_limit_bytes=56 << 20
        ),
    )(
        passage_ids.T,
        select_count,
        select_index,
        hidden.reshape(ROWS, 512),
        w_query.reshape(2, 8, 512, 256),
        w_keyvalue,
        passage_cache,
    )


def local(hidden, w_query, w_keyvalue, passage_cache, passage_ids, select_index, select_count):
    queries, begun, marks, meta, slots, incoming = exchange(
        passage_ids, select_count, select_index, hidden, w_query, w_keyvalue, passage_cache
    )
    context = attend(
        slots, select_index, select_count, queries, begun, marks, meta, incoming
    )
    return context[None]


def solution(mesh):
    placed = (
        P("store", None, "tp"),
        P(None, "tp"),
        P("tp", None),
        P("store", None, None, None),
        P(),
        P("store", None),
        P("store"),
    )
    return jax.shard_map(
        local, mesh=mesh, in_specs=placed, out_specs=P("store", None, "tp"), check_vma=False
    )
```

```python
import math

import jax
import jax.numpy as jnp
from jax import lax
from jax.experimental import pallas as pl
from jax.experimental.pallas import tpu as pltpu
from jax.sharding import PartitionSpec as P

D = 8192
KV_HEADS = 4
HEAD_DIM = 128
PASSAGE = 384
PASSAGES = 8
SEQ = 3072
ROWS = 576
ROPE_BASE = 1000000.0
EPSILON = 1e-06
BLOCK = 192
SPAN = 2 * PASSAGE
NEG = -1e30
CONTRACT = (((1,), (1,)), ((), ()))
FAR = 1 << 20


def turned(vectors, cosine, sine):
    return vectors * cosine + pltpu.roll(vectors, HEAD_DIM // 2, 1) * sine


def turn_tables(positions):
    half = HEAD_DIM // 2
    frequency = ROPE_BASE ** (-(jnp.arange(half, dtype=jnp.float32) * 2.0) / HEAD_DIM)
    angles = positions.astype(jnp.float32)[..., None] * frequency
    cosine, sine = jnp.cos(angles), jnp.sin(angles)
    return jnp.concatenate([cosine, cosine, -sine, sine], axis=-1)


def attend_kernel(
    slots_sm, pos_sm, count_sm, q_hbm, acc_hbm, marks_hbm, meta_hbm, old_table_ref, incoming_hbm,
    out_hbm, out_ref, q_s, acc_in, kp_s, meta_ref, old_ref, kk_s, vv_s, acc_s,
    sem, old_sem, out_sem,
):
    heads = q_s.shape[0]
    olds = [
        pltpu.make_async_copy(incoming_hbm.at[slots_sm[0, k]], old_ref.at[k], old_sem.at[k])
        for k in range(PASSAGES)
    ]
    fetched = [
        pltpu.make_async_copy(source, target, sem.at[i])
        for i, (source, target) in enumerate(
            ((q_hbm, q_s), (acc_hbm, acc_in), (marks_hbm, kp_s), (meta_hbm, meta_ref))
        )
    ]
    for copy in olds + fetched:
        copy.start()
    count = count_sm[0]
    vv_s[:, HEAD_DIM:] = jnp.ones_like(vv_s[:, HEAD_DIM:])
    for k in range(PASSAGES):
        olds[k].wait()
        block = old_ref[k]
        table = old_table_ref[k]
        keys = block[:, :HEAD_DIM].astype(jnp.float32)
        rows = slice(k * PASSAGE, (k + 1) * PASSAGE)
        kk_s[rows] = turned(keys, table[:, :HEAD_DIM], table[:, HEAD_DIM:]).astype(jnp.bfloat16)
        vv_s[rows, :HEAD_DIM] = block[:, HEAD_DIM:]
    for copy in fetched:
        copy.wait()
    leaving = []
    for b in range(ROWS // BLOCK):
        low, high = b * BLOCK, (b + 1) * BLOCK

        @pl.when(low >= count)
        def _():
            out_ref[low:high] = jnp.zeros_like(out_ref[low:high])

        @pl.when(low < count)
        def _():
            acc_s[...] = acc_in[b]
            tops = [acc_in[b, h * BLOCK : (h + 1) * BLOCK, 2 * HEAD_DIM - 1 :] for h in range(heads)]
            place = meta_ref[low:high, 1:2].astype(jnp.int32)
            last = jnp.minimum(count, high) - 1

            def old(i, tops):
                span = pl.ds(pl.multiple_of(i * SPAN, SPAN), SPAN)
                seen = kp_s[0:1, span] <= place
                raw = [
                    lax.dot_general(
                        q_s[h, low:high], kk_s[span], CONTRACT, preferred_element_type=jnp.float32
                    )
                    for h in range(heads)
                ]
                risen_tops = []
                for h, top in enumerate(tops):
                    mine = slice(h * BLOCK, (h + 1) * BLOCK)
                    scores = jnp.where(seen, raw[h], NEG)
                    risen = jnp.maximum(top, jnp.max(scores, axis=1, keepdims=True))
                    weight = jnp.exp2(scores - risen).astype(jnp.bfloat16)
                    part = jnp.dot(weight, vv_s[span], preferred_element_type=jnp.float32)
                    acc_s[mine] = acc_s[mine] * jnp.exp2(top - risen) + part
                    risen_tops.append(risen)
                return tuple(risen_tops)

            lax.fori_loop(0, pos_sm[0, last] // SPAN + 1, old, tuple(tops))
            result = acc_s[:, :HEAD_DIM] / acc_s[:, HEAD_DIM : HEAD_DIM + 1]
            live = low + lax.broadcasted_iota(jnp.int32, (BLOCK, HEAD_DIM), 0) < count
            for h in range(heads):
                piece = jnp.where(live, result[h * BLOCK : (h + 1) * BLOCK], 0.0)
                out_ref[low:high, h * HEAD_DIM : (h + 1) * HEAD_DIM] = piece.astype(jnp.bfloat16)

        rows = pl.ds(low, BLOCK)
        leaving.append(
            pltpu.make_async_copy(out_ref.at[rows], out_hbm.at[rows], out_sem.at[b])
        )
        leaving[b].start()
    for copy in leaving:
        copy.wait()


def attend(slots, select_index, select_count, queries, begun, marks, meta, incoming):
    heads = queries.shape[0]
    old_table = turn_tables(jnp.arange(PASSAGES) * PASSAGE)[:, None]
    smem = pl.BlockSpec(memory_space=pltpu.SMEM)
    vmem = pl.BlockSpec(memory_space=pltpu.VMEM)
    hbm = pl.BlockSpec(memory_space=pl.ANY)
    return pl.pallas_call(
        attend_kernel,
        out_shape=jax.ShapeDtypeStruct((ROWS, heads * HEAD_DIM), jnp.bfloat16),
        in_specs=[smem] * 3 + [hbm] * 4 + [vmem, hbm],
        out_specs=hbm,
        scratch_shapes=[
            pltpu.VMEM((ROWS, heads * HEAD_DIM), jnp.bfloat16),
            pltpu.VMEM(queries.shape, queries.dtype),
            pltpu.VMEM(begun.shape, begun.dtype),
            pltpu.VMEM(marks.shape, marks.dtype),
            pltpu.VMEM(meta.shape, meta.dtype),
            pltpu.VMEM((PASSAGES, PASSAGE, 2 * HEAD_DIM), jnp.bfloat16),
            pltpu.VMEM((SEQ, HEAD_DIM), jnp.bfloat16),
            pltpu.VMEM((SEQ, 2 * HEAD_DIM), jnp.bfloat16),
            pltpu.VMEM((heads * BLOCK, 2 * HEAD_DIM), jnp.float32),
            pltpu.SemaphoreType.DMA((4,)),
            pltpu.SemaphoreType.DMA((PASSAGES,)),
            pltpu.SemaphoreType.DMA((ROWS // BLOCK,)),
        ],
        name="attend",
        cost_estimate=pl.CostEstimate(flops=2 * 10**9, bytes_accessed=5 * 10**6, transcendentals=0),
        compiler_params=pltpu.CompilerParams(vmem_limit_bytes=56 << 20),
    )(slots, select_index, select_count, queries, begun, marks, meta, old_table, incoming)


RELS = (1, 7, 2, 6, 3, 5, 4)
SLOTS = (0, 1, 3, 4, 5, 6, 7)
KV_SLOT, OWN_SLOT = 2, 8
GROUPS = ((0, 3), (3, 2), (5, 2), (7, 1))
UP_SLOTS = (1, 4, 6, 7, 5, 3, 0, OWN_SLOT)
DOWN_SLOTS = (0, 3, 5, 7, 6, 4, 1, OWN_SLOT)
QUERY_FLOWS = 4
FLOWS = 6
KV_PARTS = ((0, 80), (80, 64))
SIZES = (144, 144, 144, 144, 80, 64)
ORDER = (4, 5, 0, 2, 1, 3)
ROUTES = ((1, 1), (3, 0), (2, 1), (1, 0), (3, 1), (2, 0), (0, 1))
SHARE = ROWS // QUERY_FLOWS
STEPS = 7
MESH = pl.DeviceIdType.MESH


def exchange_kernel(
    ids_ref, count_sm, pos_ref, hidden_ref, query_ref, keyvalue_ref, cache_ref,
    queries_ref, begun_ref, marks_ref, meta_ref, slots_ref, incoming_ref,
    ids_sm, held, weights, kv_own, pool, outgoing, sending, arriving, partial, squares, fresh, places,
    q_raw, table_ref, nk_s, nv_s,
    local_sem, h_send, h_recv, z_send, z_recv, k_send, k_recv,
    x_send, x_recv, f_send, f_recv, d_send, d_recv, r_send, r_recv,
    s_send, s_recv, g_send, g_recv, p_send, p_recv,
):
    store = lax.axis_index("store")
    rank = lax.axis_index("tp")
    x, high, core = store // 4, (store // 2) % 2, store % 2
    low, z = rank // 8, rank % 8
    quarter = z % 4
    head = rank // 4

    def place(to_x=x, to_core=core, to_low=low, to_z=z, to_high=high):
        return (to_x * 4 + to_high * 2 + to_core, to_low * 8 + to_z)

    def remote(source, target, send, recv, device):
        return pltpu.make_async_remote_copy(
            src_ref=source, dst_ref=target, send_sem=send, recv_sem=recv,
            device_id=device, device_id_type=MESH,
        )

    def piece(owner):
        return pl.ds(pl.multiple_of(owner * 64, 64), 64)

    locals_ = [
        pltpu.make_async_copy(hidden_ref, held.at[low], local_sem.at[0]),
        pltpu.make_async_copy(cache_ref.at[:, head], pool, local_sem.at[1]),
        pltpu.make_async_copy(query_ref.at[:, z], weights.at[OWN_SLOT], local_sem.at[2]),
    ]
    for h in range(2):
        columns = pl.ds(pl.multiple_of((low * 2 + h) * 256, 256), 256)
        locals_.append(
            pltpu.make_async_copy(
                keyvalue_ref.at[:, columns], kv_own.at[h], local_sem.at[3 + h]
            )
        )
    locals_.append(pltpu.make_async_copy(ids_ref, ids_sm, local_sem.at[6]))
    for copy in locals_:
        copy.start()

    barrier = pltpu.get_barrier_semaphore()
    for d in range(1, 16):
        pl.semaphore_signal(
            barrier, inc=1, device_id=((store + d) % 16, rank), device_id_type=MESH
        )
    for d in range(1, 8):
        pl.semaphore_signal(
            barrier, inc=1, device_id=place(to_z=(z + d) % 8), device_id_type=MESH
        )
    pl.semaphore_signal(barrier, inc=1, device_id=place(to_low=1 - low), device_id_type=MESH)
    pl.semaphore_wait(barrier, 23)

    across = place(to_low=1 - low)
    rows_of = remote(hidden_ref, held.at[low], h_send, h_recv, across)
    mine = piece(x * 2 + core)
    spread = [remote(
        query_ref.at[:, (z + 8 - rel) % 8, mine], weights.at[SLOTS[o], :, mine],
        z_send.at[o], z_recv.at[o], place(to_z=(z + 8 - rel) % 8),
    ) for o, rel in enumerate(RELS)]
    kv_rows = []
    for h in range(2):
        columns = pl.ds(pl.multiple_of(((1 - low) * 2 + h) * 256, 256), 256)
        kv_rows.append(remote(
            keyvalue_ref.at[mine, columns], weights.at[KV_SLOT, h, mine],
            k_send.at[h], k_recv.at[h], across,
        ))
    for copy in kv_rows + spread[:2] + [rows_of] + spread[2:]:
        copy.start()

    turn = 1 - 2 * core
    owners = (x, (x + 3) % 4, (x + 1) % 4, (x + 2) % 4)

    def group(g, owner):
        start, size = GROUPS[g]
        return weights.at[pl.ds(start, size), :, piece(owner * 2 + core)]

    def beside(g, way):
        to = (x + 1) % 4 if way == 0 else (x + 3) % 4
        return remote(
            group(g, x), group(g, x), x_send.at[g, way], x_recv.at[g, way], place(to_x=to)
        )

    def onward(g):
        owner = (x + 4 - turn) % 4
        to = (x + 4 + turn) % 4
        return remote(group(g, owner), group(g, owner), f_send.at[g], f_recv.at[g], place(to_x=to))

    def twin(g, i):
        block = group(g, owners[i])
        return remote(block, block, d_send.at[g, i], d_recv.at[g, i], place(to_core=1 - core))

    def first(g):
        for copy in (spread[:2] + kv_rows, spread[2:4], spread[4:6], spread[6:])[g]:
            copy.wait_recv()
        beside(g, 0).start()
        beside(g, 1).start()
        twin(g, 0).start()

    def second(g):
        beside(g, 0).wait_recv()
        beside(g, 1).wait_recv()
        onward(g).start()
        twin(g, 1).start()
        twin(g, 2).start()

    def third(g):
        onward(g).wait_recv()
        twin(g, 3).start()

    def fourth(g):
        for i in range(4):
            twin(g, i).wait_recv()

    locals_[1].wait()
    locals_[5].wait()
    for k in range(PASSAGES):
        slots_ref[0, k] = ids_sm[k, store] // 4

    def choose(d, carry):
        to = (store + d) % 16
        slot = jnp.int32(0)
        for k in range(PASSAGES):
            entry = ids_sm[k, to]
            slot = slot + jnp.where(entry // 4 == store, entry % 4, 0)
        outgoing[d] = pool[slot]
        return carry

    lax.fori_loop(0, 16, choose, 0)
    places[...] = jnp.zeros_like(places)
    places[:, :ROWS] = jnp.broadcast_to(pos_ref[...].astype(jnp.float32), (8, ROWS))
    half_dim = HEAD_DIM // 2
    lane = lax.broadcasted_iota(jnp.int32, (1, HEAD_DIM), 1)
    frequency = jnp.exp(
        (lane % half_dim).astype(jnp.float32) * (-2.0 * math.log(ROPE_BASE) / HEAD_DIM)
    )
    spot = jnp.transpose(places[...])[:ROWS, :1]
    angles = spot * frequency
    row_ids = lax.broadcasted_iota(jnp.int32, (ROWS, 1), 0)
    marked = jnp.where(row_ids < count_sm[0], spot.astype(jnp.int32), -1)
    table_ref[:, :HEAD_DIM] = jnp.cos(angles)
    table_ref[:, HEAD_DIM:] = jnp.sin(angles) * jnp.where(lane < half_dim, -1.0, 1.0)
    for k in range(PASSAGES):
        here = k * PASSAGE + lax.broadcasted_iota(jnp.int32, (1, PASSAGE), 1)
        hit = jnp.max(jnp.where(marked == here, FAR, 0), axis=0, keepdims=True)
        marks_ref[:, k * PASSAGE : (k + 1) * PASSAGE] = jnp.broadcast_to(
            jnp.maximum(here, hit), (8, PASSAGE)
        )
    nv_s[:, HEAD_DIM:] = jnp.ones_like(nv_s[:, HEAD_DIM:])
    nk_s[ROWS:] = jnp.zeros_like(nk_s[ROWS:])
    nv_s[ROWS:, :HEAD_DIM] = jnp.zeros_like(nv_s[ROWS:, :HEAD_DIM])
    keep = pltpu.make_async_copy(outgoing.at[0], incoming_ref.at[store], local_sem.at[5])
    keep.start()
    passages = []
    for other in range(2):
        for to_x, to_high in ROUTES + ((0, 0),) * other:
            to_x, to_high = (x + to_x) % 4, (high + to_high) % 2
            to = place(to_x=to_x, to_high=to_high, to_core=(core + other) % 2)
            i = len(passages)
            passages.append(remote(
                outgoing.at[(to[0] + 16 - store) % 16], incoming_ref.at[store],
                p_send.at[i], p_recv.at[i], to,
            ))

    first(0)
    first(1)
    second(0)
    first(2)
    second(1)
    first(3)
    third(0)
    second(2)
    fourth(0)
    locals_[0].wait()
    locals_[2].wait()
    locals_[3].wait()
    locals_[4].wait()
    rows_of.wait_recv()
    def slot_of(up, s):
        slots = UP_SLOTS if up else DOWN_SLOTS
        slot = slots[0]
        for i in range(1, STEPS + 1):
            slot = jnp.where(s == i, slots[i], slot)
        return slot

    def add_up(s):
        for way, (offset, size) in enumerate(KV_PARTS):
            slot = slot_of(way == 0, s)
            to = (z + 15 - s) % 8 if way == 0 else (z + 1 + s) % 8
            rows = pl.ds(way * 2 * SHARE, 2 * SHARE)
            kv_rows = pl.ds(pl.multiple_of((to % 4) * SHARE + offset, 16), size)
            total = jnp.zeros((2 * SHARE, 256), jnp.float32)
            for b in range(2):
                total += jnp.dot(held[b, rows], weights[slot, b], preferred_element_type=jnp.float32)
            partial[way, : 2 * SHARE] = total
            partial[way, 2 * SHARE : 2 * SHARE + size] = jnp.dot(
                held[low, kv_rows], kv_own[to // 4], preferred_element_type=jnp.float32
            ) + jnp.dot(
                held[1 - low, kv_rows],
                weights[KV_SLOT, to // 4],
                preferred_element_type=jnp.float32,
            )

    def is_up(f):
        return f in (0, 1, 4)

    def part_of(f):
        if f < QUERY_FLOWS:
            return partial[f // 2, f % 2 * SHARE : (f % 2 + 1) * SHARE]
        return partial[f - QUERY_FLOWS, 2 * SHARE : 2 * SHARE + SIZES[f]]

    def hop(f, s):
        to = (z + 1) % 8 if is_up(f) else (z + 7) % 8
        rows = pl.ds(0, SIZES[f])
        return remote(
            sending.at[f, s, rows], arriving.at[f, s, rows],
            r_send.at[f, s], r_recv.at[f, s], place(to_z=to),
        )

    def forward(f, s, total):
        sending[f, s, : SIZES[f]] = total.astype(jnp.bfloat16)
        hop(f, s).start()

    add_up(0)
    for f in ORDER:
        forward(f, 0, part_of(f))
    third(1)
    second(3)
    for copy in passages:
        copy.start()
    fourth(1)
    add_up(1)

    def summed(f, s):
        hop(f, s).wait_recv()
        return part_of(f) + arriving[f, s, : SIZES[f]].astype(jnp.float32)

    def relay(s):
        for f in ORDER:
            forward(f, s, summed(f, s - 1))

    relay(1)
    third(2)
    third(3)
    fourth(2)
    add_up(2)
    ones = jnp.ones((8, 512), jnp.bfloat16)
    along = (((1,), (1,)), ((), ()))
    sum_of = jnp.zeros((8, ROWS), jnp.float32)
    for b in range(2):
        wide = held[b].astype(jnp.float32)
        square = wide * wide
        upper = square.astype(jnp.bfloat16)
        lower = (square - upper.astype(jnp.float32)).astype(jnp.bfloat16)
        sum_of += lax.dot_general(ones, upper, along, preferred_element_type=jnp.float32)
        sum_of += lax.dot_general(ones, lower, along, preferred_element_type=jnp.float32)
    squares[z, :, :ROWS] = sum_of
    squares[z, :, ROWS:] = jnp.zeros((8, 640 - ROWS), jnp.float32)
    sums = [remote(
        squares.at[z], squares.at[z], s_send.at[d - 1], s_recv.at[d - 1],
        place(to_z=(z + d) % 8),
    ) for d in range(1, 8)]
    for copy in sums:
        copy.start()

    relay(2)
    fourth(3)
    add_up(3)

    def step(s, carry):
        relay(s)
        add_up(s + 1)
        return carry

    lax.fori_loop(3, STEPS, step, 0)
    for f in range(QUERY_FLOWS, FLOWS):
        offset, size = KV_PARTS[f - QUERY_FLOWS]
        fresh[quarter, offset : offset + size] = summed(f, STEPS - 1).astype(jnp.bfloat16)
    shared = [remote(
        fresh.at[quarter], fresh.at[quarter], g_send.at[d - 1], g_recv.at[d - 1],
        place(to_z=(z // 4) * 4 + (quarter + d) % 4),
    ) for d in range(1, 4)]
    for copy in shared:
        copy.start()
    for f in ORDER[2:]:
        q_raw[f * SHARE : (f + 1) * SHARE] = summed(f, STEPS - 1)
    for copy in sums:
        copy.wait_recv()
    total = squares[0]
    for b in range(1, 8):
        total += squares[b]
    inverse = lax.rsqrt(total * (1.0 / D) + EPSILON)
    first_row = lax.broadcasted_iota(jnp.int32, (8, 640), 0) == 0
    meta = jnp.transpose(jnp.where(first_row, inverse, places[...]))
    meta_ref[...] = meta
    inverse = meta[:ROWS, :1]
    heads = q_raw.shape[1] // HEAD_DIM
    scale = HEAD_DIM**-0.5 * math.log2(math.e)
    for h in range(heads):
        part = q_raw[:, h * HEAD_DIM : (h + 1) * HEAD_DIM] * inverse
        part = turned(part, table_ref[:, :HEAD_DIM], table_ref[:, HEAD_DIM:])
        queries_ref[h] = (part * scale).astype(jnp.bfloat16)
    for copy in shared:
        copy.wait_recv()
    for i in range(4):
        rows = slice(i * SHARE, (i + 1) * SHARE)
        key_value = fresh[i].astype(jnp.float32) * inverse[rows]
        key = turned(key_value[:, :HEAD_DIM], table_ref[rows, :HEAD_DIM], table_ref[rows, HEAD_DIM:])
        nk_s[rows] = key.astype(jnp.bfloat16)
        nv_s[rows, :HEAD_DIM] = key_value[:, HEAD_DIM:].astype(jnp.bfloat16)
    for b in range(ROWS // BLOCK):
        begin, end = b * BLOCK, (b + 1) * BLOCK
        width = -(-end // 128) * 128
        queries = queries_ref[:, begin:end].reshape(heads * BLOCK, HEAD_DIM)
        scores = lax.dot_general(
            queries, nk_s[:width], CONTRACT, preferred_element_type=jnp.float32
        )
        row_of = begin + lax.broadcasted_iota(jnp.int32, (BLOCK, width), 0)
        key_of = lax.broadcasted_iota(jnp.int32, (BLOCK, width), 1)
        seen = jnp.concatenate([key_of <= row_of] * heads, axis=0)
        scores = jnp.where(seen, scores, NEG)
        top = jnp.max(scores, axis=1, keepdims=True)
        weight = jnp.exp2(scores - top).astype(jnp.bfloat16)
        acc = jnp.dot(weight, nv_s[:width], preferred_element_type=jnp.float32)
        last_lane = lax.broadcasted_iota(jnp.int32, acc.shape, 1) == 2 * HEAD_DIM - 1
        begun_ref[b] = jnp.where(last_lane, top, acc)
    for copy in passages:
        copy.wait_recv()
    keep.wait()
    for copy in [rows_of] + spread + kv_rows + passages + sums + shared:
        copy.wait_send()
    for g in range(4):
        beside(g, 0).wait_send()
        beside(g, 1).wait_send()
        onward(g).wait_send()
        for i in range(4):
            twin(g, i).wait_send()

    def drained(s, carry):
        for f in range(FLOWS):
            hop(f, s).wait_send()
        return carry

    lax.fori_loop(0, STEPS, drained, 0)


def exchange(passage_ids, select_count, select_index, hidden, w_query, w_keyvalue, passage_cache):
    smem = pl.BlockSpec(memory_space=pltpu.SMEM)
    vmem = pl.BlockSpec(memory_space=pltpu.VMEM)
    hbm = pl.BlockSpec(memory_space=pltpu.HBM)
    dma = pltpu.SemaphoreType.DMA
    return pl.pallas_call(
        exchange_kernel,
        out_shape=(
            jax.ShapeDtypeStruct((2, ROWS, HEAD_DIM), jnp.bfloat16),
            jax.ShapeDtypeStruct((ROWS // BLOCK, 2 * BLOCK, 256), jnp.float32),
            jax.ShapeDtypeStruct((8, SEQ), jnp.int32),
            jax.ShapeDtypeStruct((640, 8), jnp.float32),
            jax.ShapeDtypeStruct((1, PASSAGES), jnp.int32),
            jax.ShapeDtypeStruct((16, PASSAGE, 256), jnp.bfloat16),
        ),
        in_specs=[hbm, smem, vmem, hbm, hbm, hbm, hbm],
        out_specs=(vmem, vmem, vmem, vmem, smem, pl.BlockSpec(memory_space=pl.ANY)),
        scratch_shapes=[
            pltpu.SMEM((PASSAGES, 16), jnp.int32),
            pltpu.VMEM((2, ROWS, 512), jnp.bfloat16),
            pltpu.VMEM((9, 2, 512, 256), jnp.bfloat16),
            pltpu.VMEM((2, 512, 256), jnp.bfloat16),
            pltpu.VMEM((4, PASSAGE, 256), jnp.bfloat16),
            pltpu.VMEM((16, PASSAGE, 256), jnp.bfloat16),
            pltpu.VMEM((FLOWS, STEPS, SHARE, 256), jnp.bfloat16),
            pltpu.VMEM((FLOWS, STEPS, SHARE, 256), jnp.bfloat16),
            pltpu.VMEM((2, 2 * SHARE + 80, 256), jnp.float32),
            pltpu.VMEM((8, 8, 640), jnp.float32),
            pltpu.VMEM((4, SHARE, 256), jnp.bfloat16),
            pltpu.VMEM((8, 640), jnp.float32),
            pltpu.VMEM((ROWS, 256), jnp.float32),
            pltpu.VMEM((ROWS, 2 * HEAD_DIM), jnp.float32),
            pltpu.VMEM((640, HEAD_DIM), jnp.bfloat16),
            pltpu.VMEM((640, 2 * HEAD_DIM), jnp.bfloat16),
            dma((7,)), dma(()), dma(()), dma((7,)), dma((7,)), dma((2,)), dma((2,)),
            dma((4, 2)), dma((4, 2)), dma((4,)), dma((4,)),
            dma((4, 4)), dma((4, 4)), dma((6, 7)), dma((6, 7)), dma((7,)), dma((7,)),
            dma((3,)), dma((3,)), dma((15,)), dma((15,)),
        ],
        name="exchange",
        cost_estimate=pl.CostEstimate(
            flops=3 * 10**9, bytes_accessed=10**7, transcendentals=0
        ),
        compiler_params=pltpu.CompilerParams(
            collective_id=0, has_side_effects=True, vmem_limit_bytes=56 << 20
        ),
    )(
        passage_ids.T,
        select_count,
        select_index,
        hidden.reshape(ROWS, 512),
        w_query.reshape(2, 8, 512, 256),
        w_keyvalue,
        passage_cache,
    )


def local(hidden, w_query, w_keyvalue, passage_cache, passage_ids, select_index, select_count):
    queries, begun, marks, meta, slots, incoming = exchange(
        passage_ids, select_count, select_index, hidden, w_query, w_keyvalue, passage_cache
    )
    context = attend(
        slots, select_index, select_count, queries, begun, marks, meta, incoming
    )
    return context[None]


def solution(mesh):
    placed = (
        P("store", None, "tp"),
        P(None, "tp"),
        P("tp", None),
        P("store", None, None, None),
        P(),
        P("store", None),
        P("store"),
    )
    return jax.shard_map(
        local, mesh=mesh, in_specs=placed, out_specs=P("store", None, "tp"), check_vma=False
    )
```
